32 devices in a mesh: dev: 16 (over z, y, x), rep: 2 (over core).
Axes of the slice: x: 2, y: 2, z: 4, core: 2. Of those that a mesh axis runs over, the one named last changes fastest.
Arguments:
- embeddings: float32 [4096, 4096], P(('rep', 'dev')), parts along dimension 0, may hold values from -130 to 130
- cluster_id: int32 [4096], P(('rep', 'dev')), parts along dimension 0, may hold values from 0 to 31, as said below
- member_order: int32 [4096], P(('rep', 'dev')), parts along dimension 0, may hold values from 0 to 127, as said below
- cluster_slot: int32 [64], P('rep'), parts along dimension 0, may hold values from 0 to 31, each once
- cluster_size: int32 [64], P('rep'), parts along dimension 0, may hold values from 16 to 128, as said below
Outputs:
- best_similarity: float32 [4096], P(('rep', 'dev')), parts along dimension 0
- keep: int32 [4096], P(('rep', 'dev')), parts along dimension 0
- cluster_mean: float32 [64], P(('rep', 'dev')), parts along dimension 0
The draws below stay inside these ranges and needn't reach their ends.
There are 2 independent parts, one for each index of `rep`. The reference program is written for one: setup_inputs(seed, part) draws one part's arguments, and reference() takes and returns one part's arrays. A program takes and returns all parts, laid end to end along the dimension named above; each array names one. Nothing has to cross between parts.
Inputs may be any that keep to these rules, and one draw needn't show every extreme that they name: `cluster_id`: every cluster holds at most 128 rows and some cluster exactly 128. A cluster of n members has floor(n / 16) or ceil(n / 16) of them among the rows of each device, so at most 8, a number reached on every device. `member_order`: within a cluster of n members the ranks are 0 to n - 1, each once. `cluster_slot`: a permutation; cluster c is owned by device cluster_slot[c] // 2 of dev. `cluster_size`: the number of rows whose cluster_id is c.
All inputs are finite; a program needn't handle non-finite values.
Results may differ from the reference program's by a relative error of at most 0.0003.
Values may be sent and summed in bfloat16 or wider, within the bound.
A program may use at most 64 MiB of HBM per device.

```python
import jax
import jax.numpy as jnp
from jax import lax

D = 4096
CAP = 128
CLUSTERS = 32
ROWS_ALL = 2048
N_DEV = 16


def layout(key):
    base_key = jax.random.fold_in(key, 7)
    key_sizes, key_labels, key_order, key_source, key_rows = jax.random.split(base_key, 5)
    half_count = CLUSTERS // 2
    sizes_pair = jax.random.randint(key_sizes, (half_count,), CAP // 8, CAP - CAP // 8 + 1)
    base_sizes = jnp.concatenate([sizes_pair, CAP - sizes_pair]).astype(jnp.int32)
    base_sizes = base_sizes.at[0].set(CAP).at[half_count].set(CAP // 2).at[1].set(CAP // 4).at[half_count + 1].set(CAP // 4)
    labels = jax.random.permutation(key_labels, CLUSTERS)
    sizes_out = jnp.zeros((CLUSTERS,), jnp.int32).at[labels].set(base_sizes)
    size_ends = jnp.cumsum(sizes_out)
    size_starts = size_ends - sizes_out
    positions = jnp.arange(ROWS_ALL, dtype=jnp.int32)
    owner_cluster = jnp.sum((positions[:, None] >= size_ends[None, :]).astype(jnp.int32), axis=1)
    shuffle = jax.random.permutation(key_order, ROWS_ALL).astype(jnp.int32)
    ranked = jnp.argsort(owner_cluster * ROWS_ALL + shuffle, stable=True)
    inverse = jnp.zeros((ROWS_ALL,), jnp.int32).at[ranked].set(positions)
    orders = inverse - size_starts[owner_cluster]
    source_perm = jax.random.permutation(key_source, N_DEV).astype(jnp.int32)
    source = source_perm[positions % N_DEV]
    second = jax.random.permutation(key_rows, ROWS_ALL).astype(jnp.int32)
    placed = jnp.argsort(source * ROWS_ALL + second, stable=True)
    target = jnp.zeros((ROWS_ALL,), jnp.int32).at[placed].set(positions)
    ids_out = jnp.zeros((ROWS_ALL,), jnp.int32).at[target].set(owner_cluster)
    order_out = jnp.zeros((ROWS_ALL,), jnp.int32).at[target].set(orders)
    return (ids_out, order_out, sizes_out)


def draw_cluster_id(key, part):
    return layout(key)[0]


def draw_member_order(key, part):
    return layout(key)[1]


def draw_cluster_size(key, part):
    return layout(key)[2]


def draw_embeddings(key, part):
    cluster_ids = layout(key)[0]
    base_key = jax.random.fold_in(key, 11)
    key_anchor, key_noise, key_copy = jax.random.split(base_key, 3)
    anchors = jnp.clip(jax.random.normal(key_anchor, (CLUSTERS, D), jnp.float32), -8.0, 8.0)
    noise = jnp.clip(jax.random.normal(key_noise, (ROWS_ALL, D), jnp.float32), -8.0, 8.0)
    copied = jax.random.randint(key_copy, (ROWS_ALL,), 0, 3) == 0
    values = jnp.where(copied[:, None], anchors[cluster_ids] + 0.15 * noise, noise)
    return values.astype(jnp.float32)


def setup_inputs(seed: int = 0, part: int = 0) -> dict:
    key_list = jax.random.split(jax.random.key(seed), 6)
    own_keys = jax.random.split(jax.random.fold_in(key_list[5], part), 6)
    embeddings = draw_embeddings(jax.random.fold_in(jax.random.fold_in(key_list[5], part), 71), part)
    cluster_id = draw_cluster_id(jax.random.fold_in(jax.random.fold_in(key_list[5], part), 71), part)
    member_order = draw_member_order(jax.random.fold_in(jax.random.fold_in(key_list[5], part), 71), part)
    cluster_slot = jax.random.permutation(own_keys[3], CLUSTERS).astype(jnp.int32)
    cluster_size = draw_cluster_size(jax.random.fold_in(jax.random.fold_in(key_list[5], part), 71), part)
    return {"embeddings": embeddings, "cluster_id": cluster_id, "member_order": member_order, "cluster_slot": cluster_slot, "cluster_size": cluster_size}


norm_eps = 1e-06
cutoff = 0.8

def normalized(values):
    squares_sum = lax.optimization_barrier(jnp.sum(values * values, axis=1, keepdims=True))
    return (values * lax.rsqrt(squares_sum + norm_eps)).astype(jnp.bfloat16)

def reference(embeddings, cluster_id, member_order, cluster_slot, cluster_size):
    unit_rows = normalized(embeddings)
    total_rows = embeddings.shape[0]
    where_put = (cluster_id * CAP + member_order).astype(jnp.int32)
    index_table = jnp.zeros((CLUSTERS * CAP,), jnp.int32).at[where_put].set(jnp.arange(total_rows, dtype=jnp.int32) + 1).reshape(CLUSTERS, CAP)
    spot_index = jnp.arange(CAP, dtype=jnp.int32)
    lower = spot_index[None, :] < spot_index[:, None]

    def one_cluster(packed):
        entries, size_now = packed
        occupied = entries > 0
        gathered = unit_rows[jnp.maximum(entries - 1, 0)].astype(jnp.float32)
        members = jnp.where(occupied[:, None], gathered, 0.0)
        is_live = occupied & (spot_index < size_now)
        similar = jnp.dot(members, members.T, preferred_element_type=jnp.float32)
        allowed = lower & is_live[None, :]
        nearest = lax.optimization_barrier(jnp.max(jnp.where(allowed, similar, -1.0), axis=1))
        best_spot = jnp.where(is_live, nearest, -1.0)
        mean_best = jnp.sum(jnp.where(is_live, best_spot, 0.0)) / size_now.astype(jnp.float32)
        return (best_spot, mean_best)
    best_table, cluster_means = lax.map(one_cluster, (index_table, cluster_size))
    row_best = best_table.reshape(-1)[where_put]
    keep_mask = (row_best < cutoff).astype(jnp.int32)
    by_slot = jnp.zeros((CLUSTERS,), jnp.float32).at[cluster_slot].set(cluster_means)
    return (row_best, keep_mask, by_slot)
```

```python
import functools

import jax
import jax.numpy as jnp
from jax import lax
from jax.experimental import pallas as pl
from jax.experimental.pallas import tpu as pltpu
from jax.sharding import PartitionSpec as P

CAP = 128
CHUNK = 128
LOADS = 4
WINDOW = 3
LAG = 2
DIRECT = 1
NORM_EPS = 1e-06
CUTOFF = 0.8
FIXED = 32000.0
F32 = jnp.float32
BF16 = jnp.bfloat16
I16 = jnp.int16
I32 = jnp.int32


def split_lines(n):
    z = max(z for z in range(1, n + 1) if n % z == 0 and z * z <= n)
    return z, n // z


def source_slots(n, nq, rows, group):
    largest = rows * n // nq + CAP - CAP // nq
    bound = (largest + group * (n - 1)) // n
    return min(group * -(-CAP // n), -(-bound // 16) * 16)


def iota(shape, dim):
    return lax.broadcasted_iota(I32, shape, dim)


def rows_of(values, width):
    row = iota((8, width), 0)
    out = jnp.zeros((8, width), values[0].dtype)
    for r, v in enumerate(values):
        out = jnp.where(row == r, jnp.broadcast_to(v, (8, width)), out)
    return out


def to_col(row, count):
    eye = iota((count, count), 0) == iota((count, count), 1)
    return jnp.sum(jnp.where(eye, row, 0.0), axis=1, keepdims=True)


def floor_div(x, d):
    return jnp.floor((x + 0.5) * (1.0 / d))


def kernel(n, nz, nq, emb_hbm, cid_hbm, order_hbm, slot_hbm, size_hbm, packed_out,
           emb, cid, order, slot, size, unit, line, meta, pick, packed, plane, straight, ots, otr,
           gram, own_half, hs, hr, table, units, repack,
           s_load, s_small, s_meta, r_meta, s_line, r_line, s_plane, r_plane, s_dir, r_dir,
           s_ot, r_ot, s_h, r_h, s_t, r_t):
    me = lax.axis_index("dev")
    z, q = lax.div(me, nq), lax.rem(me, nq)

    def copy(src, dst, s, r, target):
        return pltpu.make_async_remote_copy(
            src_ref=src, dst_ref=dst, send_sem=s, recv_sem=r,
            device_id={"dev": target}, device_id_type=pl.DeviceIdType.MESH)

    def on_line(d):
        return jnp.bitwise_xor(z, d) * nq + q

    def on_plane(d):
        return z * nq + jnp.bitwise_xor(q, d)

    barrier = pltpu.get_barrier_semaphore()
    friends = [on_line(d) for d in range(1, nz)] + [on_plane(d) for d in range(1, nq)]
    for t in friends:
        pl.semaphore_signal(barrier, inc=1, device_id={"dev": t},
                            device_id_type=pl.DeviceIdType.MESH)
    smalls = [pltpu.make_async_copy(a, b, s_small.at[i]) for i, (a, b) in enumerate(
        [(cid_hbm, cid), (order_hbm, order), (slot_hbm, slot), (size_hbm, size)])]
    parts = s_load.shape[0]
    tall = emb.shape[0] // parts
    loads = [pltpu.make_async_copy(emb_hbm.at[pl.ds(i * tall, tall)], emb.at[pl.ds(i * tall, tall)],
                                   s_load.at[i]) for i in range(parts)]
    for c in smalls + loads:
        c.start()
    rows = emb.shape[0]
    clusters = slot.shape[1]
    per_owner = clusters // n
    chunks, width = line.shape[0], line.shape[3]
    group = nz * per_owner
    slots = plane.shape[2] // nz
    half = CAP // 2
    lined = chunks - DIRECT

    for c in smalls:
        c.wait()
    slot_c = to_col(slot[...].astype(F32), clusters)
    size_r = size[...].astype(F32)
    size_c = to_col(size_r, clusters)
    c_row, c_col = iota((clusters, clusters), 1), iota((clusters, clusters), 0)
    ahead = (size_r > size_c) | ((size_r == size_c) & (c_row < c_col))
    place_in = jnp.sum(jnp.where(ahead, 1.0, 0.0), axis=1, keepdims=True)
    e_c = floor_div(place_in, nq)
    turn = place_in - e_c * nq
    odd = e_c - 2.0 * floor_div(e_c, 2)
    g_c = jnp.where(odd > 0.5, nq - 1 - turn, turn)
    oz_c = floor_div(e_c, per_owner)
    local_c = e_c - oz_c * per_owner
    work_c = (oz_c * nq + g_c) * per_owner + local_c
    is_mem = iota((clusters, rows), 0) == cid[...]

    def of_row(v):
        return jnp.sum(jnp.where(is_mem, v, 0.0), axis=0, keepdims=True)

    e_row, work_row = of_row(e_c), of_row(work_c).astype(I32)
    rel = jnp.bitwise_xor(of_row(g_c).astype(I32), q)
    tri = (iota((rows, rows), 0) < iota((rows, rows), 1)).astype(F32).astype(BF16)
    wide_q = -(-nq // 16) * 16
    in_group = iota((wide_q, rows), 0) == rel
    before = jnp.dot(in_group.astype(F32).astype(BF16), tri, preferred_element_type=F32)
    rank = jnp.sum(jnp.where(in_group, before, 0.0), axis=0, keepdims=True)
    place = rel.astype(F32) * slots + rank
    ord_row = order[...].astype(F32)
    meta[0] = rows_of([place, ord_row + 1.0, e_row + 1.0], rows)

    sums = []
    for i in range(parts):
        loads[i].wait()
        x = emb[i * tall:(i + 1) * tall, :]
        sums.append(jnp.sum(x * x, axis=1, keepdims=True))
    scale = lax.rsqrt(jnp.concatenate(sums, axis=0) + NORM_EPS)

    lines, planes = [], []
    line_order = [d for d in (2, 3, 1) if d < nz] + list(range(4, nz))

    def make_unit(k):
        for t in range(nz):
            c0 = (t * chunks + k) * width
            unit[t, k] = (emb[:, c0:c0 + width] * scale).astype(BF16)

    def send_line(k):
        make_unit(k)
        now = [copy(unit.at[jnp.bitwise_xor(z, d), k], line.at[k, d], s_line.at[k, d], r_line.at[k, d], on_line(d))
               for d in line_order]
        for c in now:
            c.start()
        line[k, 0] = unit[z, k]
        lines.append(now)

    pl.semaphore_wait(barrier, len(friends))
    metas = [copy(meta.at[0], meta.at[d], s_meta.at[d], r_meta.at[d], on_line(d)) for d in range(1, nz)]
    for c in metas:
        c.start()
    for k in range(min(WINDOW, lined)):
        send_line(k)

    def label(d):
        pick[d] = jnp.where(iota((nq * slots, rows), 0) == meta[d, 0:1, :].astype(I32), 1.0, 0.0).astype(BF16)
        values = jnp.where((iota((8, rows), 0) == 1) | (iota((8, rows), 0) == 2), meta[d], 0.0).astype(BF16)
        return lax.dot_general(values, pick[d], (((1,), (1,)), ((), ())), preferred_element_type=F32)

    told = [label(0)]
    if DIRECT:
        make_unit(chunks - 1)
        for t in range(nz):
            got = jnp.dot(pick[0], unit[t, chunks - 1], preferred_element_type=F32).astype(BF16)
            straight[t] = got.reshape(nq, slots, width)
        plane[chunks - 1, 0, 0:slots] = straight[z, 0]
    for d, c in enumerate(metas):
        c.wait_recv()
        told.append(label(d + 1))
    for d in range(nq):
        ots[d] = jnp.concatenate([v[:, d * slots:(d + 1) * slots] for v in told], axis=1)
    orders = [copy(ots.at[d], otr.at[d], s_ot.at[d], r_ot.at[d], on_plane(d)) for d in range(1, nq)]
    for c in orders:
        c.start()

    def make_repack():
        for c in orders:
            c.wait_recv()
        labs = jnp.concatenate([ots[0]] + [otr[d] for d in range(1, nq)], axis=1)
        target = ((labs[2:3, :] - 1.0) * CAP + labs[1:2, :] - 1.0).astype(I32)

        def one(e, _):
            hit = iota((CAP, n * slots), 0) + e * CAP == target
            repack[e] = jnp.where(hit, 1.0, 0.0).astype(BF16)
            return 0

        lax.fori_loop(0, group, one, 0)

    directs = []
    spans = [list(range(k, min(k + 2, chunks))) for k in range(0, chunks, 2)]
    below = iota((half, CAP), 0) + half > iota((half, CAP), 1)

    def arrived(span):
        if span[0] == 0:
            make_repack()
        for k in span:
            for c in planes[k] if k < lined else directs:
                c.wait_recv()
        blocks = [plane[k].reshape(n * slots, width) for k in span]
        return blocks[0] if len(blocks) == 1 else jnp.concatenate(blocks, axis=1)

    def partial_gram(m):
        return lax.dot_general(m, m, (((1,), (1,)), ((), ())), preferred_element_type=F32)

    def add_gram(span):
        block = arrived(span)
        got = jnp.dot(repack[...].reshape(group * CAP, n * slots), block, preferred_element_type=F32)
        units[:, :, :block.shape[1]] = got.astype(BF16).reshape(group, CAP, block.shape[1])
        for e in range(group):
            s = partial_gram(units[e, :, :block.shape[1]])
            gram[e] = s if span[0] == 0 else gram[e] + s

    done = 0
    for k in range(lined):
        for c in lines[k]:
            c.wait_recv()
        if k + WINDOW < lined:
            send_line(k + WINDOW)
        if DIRECT and k == max(lined - 2, 0):
            for d in range(1, n):
                dz, dq = divmod(d, nq)
                directs.append(copy(straight.at[jnp.bitwise_xor(z, dz), dq],
                                    plane.at[chunks - 1, dq, pl.ds(dz * slots, slots)],
                                    s_dir.at[d], r_dir.at[d],
                                    jnp.bitwise_xor(z, dz) * nq + jnp.bitwise_xor(q, dq)))
            for c in directs:
                c.start()
        for d in range(nz):
            got = jnp.dot(pick[d], line[k, d], preferred_element_type=F32).astype(BF16)
            plane[k, 0, d * slots:(d + 1) * slots] = got[:slots]
            packed[k, :, d * slots:(d + 1) * slots] = got[slots:].reshape(nq - 1, slots, width)
        now = [copy(packed.at[k, d - 1], plane.at[k, d], s_plane.at[k, d], r_plane.at[k, d], on_plane(d))
               for d in range(nq - 1, 0, -1)]
        for c in now:
            c.start()
        planes.append(now)
        if done < len(spans) - 1 and spans[done][-1] + LAG <= k:
            add_gram(spans[done])
            done += 1
    while done < len(spans) - 1:
        add_gram(spans[done])
        done += 1

    block = arrived(spans[-1])
    wide = block.shape[1]
    halves = []
    for d in list(range(nz - 1, 0, -1)) + [0]:
        first = jnp.bitwise_xor(z, d) * per_owner
        got = jnp.dot(repack[pl.ds(first, per_owner)].reshape(per_owner * CAP, n * slots), block,
                      preferred_element_type=F32).astype(BF16)
        for l in range(per_owner):
            full = partial_gram(got[l * CAP:(l + 1) * CAP])
            if len(spans) > 1:
                full = full + gram[first + l]
            part = jnp.where(below, full[half:, :], pltpu.roll(full[:half, :], half, 1))
            if d:
                hs[d, l] = jnp.round(part * FIXED).astype(I32).astype(I16)
            else:
                own_half[l] = part
        if d:
            c = copy(hs.at[d], hr.at[d], s_h.at[d], r_h.at[d], on_line(d))
            c.start()
            halves.append(c)
    for group_of in [metas, orders, directs] + lines + planes:
        for c in group_of:
            c.wait_send()

    lane = iota((1, CAP), 1)
    at = jnp.where(lane < half, lane + half, lane - half).astype(F32)
    up_row = iota((half, CAP), 0)
    up_col = iota((half, CAP), 1)
    mine = [(me * per_owner + l).astype(F32) for l in range(per_owner)]
    n_mem = [jnp.sum(jnp.where(work_c == m, size_c, 0.0), axis=0, keepdims=True) for m in mine]
    for c in halves:
        c.wait_recv()
    bests, means = [], []
    for l in range(per_owner):
        far = hr[1, l].astype(I32)
        for d in range(2, nz):
            far = far + hr[d, l].astype(I32)
        p = own_half[l] + far.astype(F32) * (1.0 / FIXED)
        low = jnp.max(jnp.where(below & (up_col.astype(F32) < n_mem[l]), p, -1.0), axis=1, keepdims=True)
        low = jnp.max(jnp.where(up_row == up_col, low, -1.0), axis=0, keepdims=True)
        top_ok = (up_row + half < up_col) & (up_row.astype(F32) < n_mem[l])
        top = jnp.max(jnp.where(top_ok, p, -1.0), axis=0, keepdims=True)
        near = jnp.where(lane < half, low, top)
        live = at < n_mem[l]
        bests.append(jnp.where(live, near, -1.0))
        means.append(jnp.sum(jnp.where(live, near, 0.0), axis=1, keepdims=True) / n_mem[l])
    lanes = jnp.zeros((1, CAP), F32)
    for l in range(per_owner):
        lanes = jnp.where(lane == l, means[l], lanes)
    table[me] = rows_of(bests + [lanes], CAP)[:table.shape[1], :]
    backs = [copy(table.at[me], table.at[me], s_t.at[d], r_t.at[d], jnp.bitwise_xor(me, d))
             for d in range(n - 1, 0, -1)]
    for c in backs:
        c.start()
    pos = order[...]
    pos = jnp.where(pos < half, pos + half, pos - half)
    hot = jnp.where(iota((clusters, rows), 0) == work_row, 1.0, 0.0)
    for c in halves:
        c.wait_send()
    for c in backs:
        c.wait_recv()
    full = table[...]
    flat = full[:, :per_owner, :].reshape(clusters, CAP).T
    told = full[:, per_owner:per_owner + 1, :].reshape(n, CAP)
    mean = jnp.zeros((1, rows), F32)
    for l in range(per_owner):
        work = jnp.sum(jnp.where(slot_c == mine[l], work_c, 0.0), axis=0, keepdims=True).astype(I32)
        hit = iota((n, CAP), 0) * per_owner + iota((n, CAP), 1) == work
        hit = hit & (iota((n, CAP), 1) < per_owner)
        part = jnp.sum(jnp.where(hit, told, 0.0), axis=1, keepdims=True)
        mean = jnp.where(iota((1, rows), 1) == l, jnp.sum(part, axis=0, keepdims=True), mean)
    got = jnp.dot(flat, hot, preferred_element_type=F32, precision=lax.Precision.HIGHEST)
    out = jnp.sum(jnp.where(iota((CAP, rows), 0) == pos, got, 0.0), axis=0, keepdims=True)
    packed_out[...] = rows_of([out, mean], rows)
    for c in backs:
        c.wait_send()


def finish(packed, best_out, keep_out, mean_out):
    best = packed[0:1, :]
    best_out[...] = best
    keep_out[...] = jnp.where(best < CUTOFF, 1, 0)
    mean_out[...] = packed[1:2, :mean_out.shape[1]]


def body(embeddings, cluster_id, member_order, cluster_slot, cluster_size):
    n = lax.axis_size("dev")
    nz, nq = split_lines(n)
    rows, depth = embeddings.shape
    clusters = cluster_slot.shape[0]
    per_owner = clusters // n
    width = min(CHUNK, depth // nz)
    chunks = depth // nz // width
    group = nz * per_owner
    slots = source_slots(n, nq, rows, group)
    half = CAP // 2
    vmem = pl.BlockSpec(memory_space=pltpu.VMEM)
    dma = pltpu.SemaphoreType.DMA
    packed = pl.pallas_call(
        functools.partial(kernel, n, nz, nq),
        out_shape=jax.ShapeDtypeStruct((8, rows), F32),
        in_specs=[pl.BlockSpec(memory_space=pl.ANY)] * 5,
        out_specs=vmem,
        scratch_shapes=[
            pltpu.VMEM((rows, depth), F32),
            pltpu.VMEM((1, rows), I32),
            pltpu.VMEM((1, rows), I32),
            pltpu.VMEM((1, clusters), I32),
            pltpu.VMEM((1, clusters), I32),
            pltpu.VMEM((nz, chunks, rows, width), BF16),
            pltpu.VMEM((chunks, nz, rows, width), BF16),
            pltpu.VMEM((nz, 8, rows), F32),
            pltpu.VMEM((nz, nq * slots, rows), BF16),
            pltpu.VMEM((chunks, nq - 1, nz * slots, width), BF16),
            pltpu.VMEM((chunks, nq, nz * slots, width), BF16),
            pltpu.VMEM((nz, nq, slots, width), BF16),
            pltpu.VMEM((nq, 8, nz * slots), F32),
            pltpu.VMEM((nq, 8, nz * slots), F32),
            pltpu.VMEM((group, CAP, CAP), F32),
            pltpu.VMEM((per_owner, half, CAP), F32),
            pltpu.VMEM((nz, per_owner, half, CAP), I16),
            pltpu.VMEM((nz, per_owner, half, CAP), I16),
            pltpu.VMEM((n, pl.next_power_of_2(per_owner + 1), CAP), F32),
            pltpu.VMEM((group, CAP, 2 * width), BF16),
            pltpu.VMEM((group, CAP, n * slots), BF16),
            dma((LOADS,)), dma((4,)),
            dma((nz,)), dma((nz,)),
            dma((chunks, nz)), dma((chunks, nz)),
            dma((chunks, nq)), dma((chunks, nq)),
            dma((n,)), dma((n,)),
            dma((nq,)), dma((nq,)),
            dma((nz,)), dma((nz,)),
            dma((n,)), dma((n,)),
        ],
        compiler_params=pltpu.CompilerParams(
            collective_id=0, has_side_effects=True, vmem_limit_bytes=62 * 1024 * 1024),
    )(embeddings, cluster_id.reshape(1, rows), member_order.reshape(1, rows),
      cluster_slot.reshape(1, clusters), cluster_size.reshape(1, clusters))
    best, keep, mean = pl.pallas_call(
        finish,
        out_shape=(jax.ShapeDtypeStruct((1, rows), F32), jax.ShapeDtypeStruct((1, rows), I32),
                   jax.ShapeDtypeStruct((1, per_owner), F32)),
        in_specs=[vmem],
        out_specs=(vmem,) * 3,
    )(packed)
    return best.reshape(rows), keep.reshape(rows), mean.reshape(per_owner)


def solution(mesh):
    placed = (P(("rep", "dev"), None), P(("rep", "dev")), P(("rep", "dev")), P("rep"), P("rep"))
    return jax.shard_map(
        body,
        mesh=mesh,
        in_specs=placed,
        out_specs=(P(("rep", "dev")), P(("rep", "dev")), P(("rep", "dev"))),
        check_vma=False,
    )
```

```python
import functools

import jax
import jax.numpy as jnp
from jax import lax
from jax.experimental import pallas as pl
from jax.experimental.pallas import tpu as pltpu
from jax.sharding import PartitionSpec as P

CAP = 128
CHUNK = 128
LOADS = 4
FAR_AHEAD = 4
SLOW = 2
LAG = 2
STRAIGHT = 1
NORM_EPS = 1e-06
CUTOFF = 0.8
META, ORDER, LINE, PLANE, DIRECT, HALF, BACK = range(7)
FIXED = 32000.0
F32 = jnp.float32
BF16 = jnp.bfloat16
I16 = jnp.int16
I32 = jnp.int32


def split_lines(n):
    z = max(z for z in range(1, n + 1) if n % z == 0 and z * z <= n)
    return z, n // z


def source_slots(n, nq, rows, group):
    largest = rows * n // nq + CAP - CAP // nq
    bound = (largest + group * (n - 1)) // n
    return min(group * -(-CAP // n), -(-bound // 16) * 16)


def iota(shape, dim):
    return lax.broadcasted_iota(I32, shape, dim)


def rows_of(values, width):
    row = iota((8, width), 0)
    out = jnp.zeros((8, width), values[0].dtype)
    for r, v in enumerate(values):
        out = jnp.where(row == r, jnp.broadcast_to(v, (8, width)), out)
    return out


def to_col(row, count):
    eye = iota((count, count), 0) == iota((count, count), 1)
    return jnp.sum(jnp.where(eye, row, 0.0), axis=1, keepdims=True)


def floor_div(x, d):
    return jnp.floor((x + 0.5) * (1.0 / d))


def kernel(n, nz, nq, emb_hbm, cid_hbm, order_hbm, slot_hbm, size_hbm, packed_out,
           emb, cid, order, slot, size, unit, line, meta, pick, packed, plane, straight, ots, otr,
           acc, hs, hr, table, units, repack,
           s_load, s_small, r_line, r_plane, sent, came):
    me = lax.axis_index("dev")
    z, q = lax.div(me, nq), lax.rem(me, nq)

    def copy(src, dst, s, r, target):
        return pltpu.make_async_remote_copy(
            src_ref=src, dst_ref=dst, send_sem=s, recv_sem=r,
            device_id={"dev": target}, device_id_type=pl.DeviceIdType.MESH)

    def arrive(ref, sem):
        pltpu.make_async_copy(ref, ref, sem).wait()

    def on_line(d):
        return jnp.bitwise_xor(z, d) * nq + q

    def on_plane(d):
        return z * nq + jnp.bitwise_xor(q, d)

    barrier = pltpu.get_barrier_semaphore()
    friends = [on_line(d) for d in range(1, nz)] + [on_plane(d) for d in range(1, nq)]
    for t in friends:
        pl.semaphore_signal(barrier, inc=1, device_id={"dev": t},
                            device_id_type=pl.DeviceIdType.MESH)
    smalls = [pltpu.make_async_copy(a, b, s_small.at[i]) for i, (a, b) in enumerate(
        [(cid_hbm, cid), (order_hbm, order), (slot_hbm, slot), (size_hbm, size)])]
    parts = s_load.shape[0]
    tall = emb.shape[0] // parts
    loads = [pltpu.make_async_copy(emb_hbm.at[pl.ds(i * tall, tall)], emb.at[pl.ds(i * tall, tall)],
                                   s_load.at[i]) for i in range(parts)]
    for c in smalls + loads:
        c.start()
    rows = emb.shape[0]
    clusters = slot.shape[1]
    per_owner = clusters // n
    chunks, width = line.shape[0], line.shape[3]
    group = nz * per_owner
    per_hub = group // 2
    first_hub = nz // 2 - 1
    slots = plane.shape[2] // nz
    half = CAP // 2
    lined = chunks - STRAIGHT

    for c in smalls:
        c.wait()
    slot_c = to_col(slot[...].astype(F32), clusters)
    size_r = size[...].astype(F32)
    size_c = to_col(size_r, clusters)
    c_row, c_col = iota((clusters, clusters), 1), iota((clusters, clusters), 0)
    ahead = (size_r > size_c) | ((size_r == size_c) & (c_row < c_col))
    place_in = jnp.sum(jnp.where(ahead, 1.0, 0.0), axis=1, keepdims=True)
    e_c = floor_div(place_in, nq)
    turn = place_in - e_c * nq
    odd = e_c - 2.0 * floor_div(e_c, 2)
    g_c = jnp.where(odd > 0.5, nq - 1 - turn, turn)
    hub_c = floor_div(e_c, per_hub)
    work_c = (hub_c * nq + g_c) * per_hub + e_c - hub_c * per_hub
    is_mem = iota((clusters, rows), 0) == cid[...]

    def of_row(v):
        return jnp.sum(jnp.where(is_mem, v, 0.0), axis=0, keepdims=True)

    e_row, work_row = of_row(e_c), of_row(work_c).astype(I32)
    rel = jnp.bitwise_xor(of_row(g_c).astype(I32), q)
    tri = (iota((rows, rows), 0) < iota((rows, rows), 1)).astype(F32).astype(BF16)
    wide_q = -(-nq // 16) * 16
    in_group = iota((wide_q, rows), 0) == rel
    before = jnp.dot(in_group.astype(F32).astype(BF16), tri, preferred_element_type=F32)
    rank = jnp.sum(jnp.where(in_group, before, 0.0), axis=0, keepdims=True)
    place = rel.astype(F32) * slots + rank
    ord_row = order[...].astype(F32)
    meta[0] = rows_of([place, ord_row + 1.0, e_row + 1.0], rows)

    sums = []
    for i in range(parts):
        loads[i].wait()
        x = emb[i * tall:(i + 1) * tall, :]
        sums.append(jnp.sum(x * x, axis=1, keepdims=True))
    scale = lax.rsqrt(jnp.concatenate(sums, axis=0) + NORM_EPS)

    line_order = [d for d in (2, 3, 1) if d < nz] + list(range(4, nz))

    def make_unit(k):
        for t in range(nz):
            c0 = (t * chunks + k) * width
            unit[t, k] = (emb[:, c0:c0 + width] * scale).astype(BF16)

    def send_line(k):
        for d in line_order:
            copy(unit.at[jnp.bitwise_xor(z, d), k], line.at[k, d], sent.at[LINE], r_line.at[k], on_line(d)).start()
        line[k, 0] = unit[z, k]

    pl.semaphore_wait(barrier, len(friends))
    for d in range(1, nz):
        copy(meta.at[0], meta.at[d], sent.at[META], came.at[META], on_line(d)).start()
    far = lax.axis_index("rep") == 0
    for k in range(chunks):
        make_unit(k)
        if k < min(FAR_AHEAD, lined):
            pl.when(far | (k == 0))(functools.partial(send_line, k))
    def label(d):
        pick[d] = jnp.where(iota((nq * slots, rows), 0) == meta[d, 0:1, :].astype(I32), 1.0, 0.0).astype(BF16)
        values = jnp.where((iota((8, rows), 0) == 1) | (iota((8, rows), 0) == 2), meta[d], 0.0).astype(BF16)
        return lax.dot_general(values, pick[d], (((1,), (1,)), ((), ())), preferred_element_type=F32)

    told = [label(0)]
    if STRAIGHT:
        for t in range(nz):
            got = jnp.dot(pick[0], unit[t, chunks - 1], preferred_element_type=F32).astype(BF16)
            straight[t * nq:(t + 1) * nq] = got.reshape(nq, slots, width)
        plane[chunks - 1, 0, 0:slots] = straight[z * nq]
    arrive(meta.at[pl.ds(1, nz - 1)], came.at[META])
    told += [label(d) for d in range(1, nz)]
    for d in range(nq):
        ots[d] = jnp.concatenate([v[:, d * slots:(d + 1) * slots] for v in told], axis=1)
    for d in range(1, nq):
        copy(ots.at[d], otr.at[d], sent.at[ORDER], came.at[ORDER], on_plane(d)).start()

    def make_repack():
        arrive(otr.at[pl.ds(1, nq - 1)], came.at[ORDER])
        labs = jnp.concatenate([ots[0]] + [otr[d] for d in range(1, nq)], axis=1)
        target = ((labs[2:3, :] - 1.0) * CAP + labs[1:2, :] - 1.0).astype(I32)

        def one(e, _):
            hit = iota((CAP, n * slots), 0) + e * CAP == target
            repack[e] = jnp.where(hit, 1.0, 0.0).astype(BF16)
            return 0

        lax.fori_loop(0, group, one, 0)

    pair = 2 if chunks % 2 == 0 else 1
    spans = chunks // pair
    below = iota((half, CAP), 0) + half > iota((half, CAP), 1)
    acc[...] = jnp.zeros(acc.shape, F32)

    def take_line(k):
        arrive(line.at[k, pl.ds(1, nz - 1)], r_line.at[k])

        @pl.when(jnp.logical_not(far) & (k == SLOW) & (k + 1 < lined))
        def _():
            send_line(k + 1)

        ahead = jnp.where(far, FAR_AHEAD, jnp.where(k < SLOW, 1, 2))

        @pl.when(k + ahead < lined)
        def _():
            send_line(k + ahead)

        if STRAIGHT:
            @pl.when(k == max(lined - 3, 0))
            def _():
                for d in range(1, n):
                    dz, dq = divmod(d, nq)
                    copy(straight.at[jnp.bitwise_xor(z, dz) * nq + dq],
                         plane.at[chunks - 1, dq, pl.ds(dz * slots, slots)],
                         sent.at[DIRECT], came.at[DIRECT], jnp.bitwise_xor(z, dz) * nq + jnp.bitwise_xor(q, dq)).start()

        for d in range(nz):
            got = jnp.dot(pick[d], line[k, d], preferred_element_type=F32).astype(BF16)
            plane[k, 0, d * slots:(d + 1) * slots] = got[:slots]
            packed[k, :, d * slots:(d + 1) * slots] = got[slots:].reshape(nq - 1, slots, width)
        for d in range(nq - 1, 0, -1):
            copy(packed.at[k, d - 1], plane.at[k, d], sent.at[PLANE], r_plane.at[k], on_plane(d)).start()

    def take_span(j):
        for i in range(pair):
            k = j * pair + i

            @pl.when(k < lined)
            def _():
                arrive(plane.at[k, pl.ds(1, nq - 1)], r_plane.at[k])

            if STRAIGHT:
                @pl.when(k == lined)
                def _():
                    arrive(straight.at[pl.ds(1, n - 1)], came.at[DIRECT])
        block = [plane[j * pair + i].reshape(n * slots, width) for i in range(pair)]
        block = jnp.concatenate(block, axis=1) if pair > 1 else block[0]
        got = jnp.dot(repack[...].reshape(group * CAP, n * slots), block, preferred_element_type=F32)
        units[...] = got.astype(BF16).reshape(units.shape)

        for b in range(group // 2):
            m = units[b]
            s = lax.dot_general(m, m, (((1,), (1,)), ((), ())), preferred_element_type=F32)
            for l in range(2):
                full = s[l * CAP:(l + 1) * CAP, l * CAP:(l + 1) * CAP]
                part = acc[2 * b + l] + jnp.where(below, full[half:, :], pltpu.roll(full[:half, :], half, 1))
                acc[2 * b + l] = part
                hs[2 * b + l] = jnp.round(part * FIXED).astype(I32).astype(I16)

        @pl.when(j == spans - 1)
        def _():
            for i in range(2):
                h = jnp.where(z > first_hub, i, 1 - i)

                @pl.when(z != first_hub + h)
                def _():
                    copy(hs.at[pl.ds(h * per_hub, per_hub)], hr.at[jnp.bitwise_xor(z, first_hub + h)],
                         sent.at[HALF], came.at[HALF], (first_hub + h) * nq + q).start()

    def step(k, _):
        @pl.when(k < lined)
        def _():
            take_line(k)

        @pl.when(k == min(lined, pair + LAG - 1) - 1)
        def _():
            make_repack()

        back = k - LAG - (pair - 1)

        @pl.when((back >= 0) & (lax.rem(back, pair) == 0))
        def _():
            take_span(lax.div(back, pair))
        return 0

    lax.fori_loop(0, pair * spans + LAG, step, 0)
    arrive(meta.at[pl.ds(1, nz - 1)], sent.at[META])
    arrive(ots.at[pl.ds(1, nq - 1)], sent.at[ORDER])
    arrive(line.at[pl.ds(0, lined), pl.ds(1, nz - 1)], sent.at[LINE])
    arrive(packed.at[pl.ds(0, lined)], sent.at[PLANE])
    if STRAIGHT:
        arrive(straight.at[pl.ds(1, n - 1)], sent.at[DIRECT])

    lane = iota((1, CAP), 1)
    at = jnp.where(lane < half, lane + half, lane - half).astype(F32)
    up_row = iota((half, CAP), 0)
    up_col = iota((half, CAP), 1)
    is_hub = (z == first_hub) | (z == first_hub + 1)
    hub = (z - first_hub) * nq + q

    @pl.when(is_hub)
    def _():
        own = (z - first_hub) * per_hub
        n_mem = []
        for l in range(per_hub):
            w = (hub * per_hub + l).astype(F32)
            n_mem.append(jnp.sum(jnp.where(work_c == w, size_c, 0.0), axis=0, keepdims=True))
        arrive(hr.at[pl.ds(1, nz - 1)], came.at[HALF])
        for l in range(per_hub):
            apart = hr[1, l].astype(I32)
            for d in range(2, nz):
                apart = apart + hr[d, l].astype(I32)
            p = acc[own + l] + apart.astype(F32) * (1.0 / FIXED)
            low = jnp.max(jnp.where(below & (up_col.astype(F32) < n_mem[l]), p, -1.0), axis=1, keepdims=True)
            low = jnp.max(jnp.where(up_row == up_col, low, -1.0), axis=0, keepdims=True)
            top_ok = (up_row + half < up_col) & (up_row.astype(F32) < n_mem[l])
            top = jnp.max(jnp.where(top_ok, p, -1.0), axis=0, keepdims=True)
            live = at < n_mem[l]
            near = jnp.where(live, jnp.where(lane < half, low, top), -1.0)
            mean = jnp.sum(jnp.where(live, near, 0.0), axis=1, keepdims=True) / n_mem[l]
            table[hub, l:l + 1] = jnp.where(lane == half, mean, near)
        for d in range(n - 1, 0, -1):
            copy(table.at[hub], table.at[hub], sent.at[BACK], came.at[BACK], jnp.bitwise_xor(me, d)).start()

    pos = order[...]
    pos = jnp.where(pos < half, pos + half, pos - half)
    hot = jnp.where(iota((clusters, rows), 0) == work_row, 1.0, 0.0)
    hubs = table.shape[0]

    @pl.when(is_hub)
    def _():
        arrive(hs.at[pl.ds(0, per_hub)], sent.at[HALF])
        arrive(table.at[pl.ds(0, hubs - 1)], came.at[BACK])

    @pl.when(jnp.logical_not(is_hub))
    def _():
        arrive(hs, sent.at[HALF])
        arrive(table, came.at[BACK])

    flat = table[...].reshape(clusters, CAP)
    mean = jnp.zeros((1, rows), F32)
    for l in range(per_owner):
        work = jnp.sum(jnp.where(slot_c == (me * per_owner + l).astype(F32), work_c, 0.0), axis=0, keepdims=True).astype(I32)
        hit = (iota((clusters, CAP), 0) == work) & (iota((clusters, CAP), 1) == half)
        part = jnp.sum(jnp.where(hit, flat, 0.0), axis=1, keepdims=True)
        mean = jnp.where(iota((1, rows), 1) == l, jnp.sum(part, axis=0, keepdims=True), mean)
    got = jnp.dot(flat.T, hot, preferred_element_type=F32, precision=lax.Precision.HIGHEST)
    out = jnp.sum(jnp.where(iota((CAP, rows), 0) == pos, got, 0.0), axis=0, keepdims=True)
    out = jnp.where(order[...] == 0, -1.0, out)
    packed_out[...] = rows_of([out, mean], rows)
    @pl.when(is_hub)
    def _():
        for d in range(0, n - 1, hubs - 1):
            arrive(table.at[pl.ds(0, min(hubs - 1, n - 1 - d))], sent.at[BACK])


def finish(packed, best_out, keep_out, mean_out):
    best = packed[0:1, :]
    best_out[...] = best
    keep_out[...] = jnp.where(best < CUTOFF, 1, 0)
    mean_out[...] = packed[1:2, :mean_out.shape[1]]


def body(embeddings, cluster_id, member_order, cluster_slot, cluster_size):
    n = lax.axis_size("dev")
    nz, nq = split_lines(n)
    rows, depth = embeddings.shape
    clusters = cluster_slot.shape[0]
    per_owner = clusters // n
    width = min(CHUNK, depth // nz)
    chunks = depth // nz // width
    group = nz * per_owner
    slots = source_slots(n, nq, rows, group)
    pair = 2 if chunks % 2 == 0 else 1
    half = CAP // 2
    vmem = pl.BlockSpec(memory_space=pltpu.VMEM)
    dma = pltpu.SemaphoreType.DMA
    packed = pl.pallas_call(
        functools.partial(kernel, n, nz, nq),
        out_shape=jax.ShapeDtypeStruct((8, rows), F32),
        in_specs=[pl.BlockSpec(memory_space=pl.ANY)] * 5,
        out_specs=vmem,
        scratch_shapes=[
            pltpu.VMEM((rows, depth), F32),
            pltpu.VMEM((1, rows), I32),
            pltpu.VMEM((1, rows), I32),
            pltpu.VMEM((1, clusters), I32),
            pltpu.VMEM((1, clusters), I32),
            pltpu.VMEM((nz, chunks, rows, width), BF16),
            pltpu.VMEM((chunks, nz, rows, width), BF16),
            pltpu.VMEM((nz, 8, rows), F32),
            pltpu.VMEM((nz, nq * slots, rows), BF16),
            pltpu.VMEM((chunks, nq - 1, nz * slots, width), BF16),
            pltpu.VMEM((chunks, nq, nz * slots, width), BF16),
            pltpu.VMEM((n, slots, width), BF16),
            pltpu.VMEM((nq, 8, nz * slots), F32),
            pltpu.VMEM((nq, 8, nz * slots), F32),
            pltpu.VMEM((group, half, CAP), F32),
            pltpu.VMEM((group, half, CAP), I16),
            pltpu.VMEM((nz, group // 2, half, CAP), I16),
            pltpu.VMEM((2 * nq, group // 2, CAP), F32),
            pltpu.VMEM((group // 2, 2 * CAP, pair * width), BF16),
            pltpu.VMEM((group, CAP, n * slots), BF16),
            dma((LOADS,)), dma((4,)), dma((chunks,)), dma((chunks,)), dma((7,)), dma((7,)),
        ],
        compiler_params=pltpu.CompilerParams(
            collective_id=0, has_side_effects=True, vmem_limit_bytes=62 * 1024 * 1024),
    )(embeddings, cluster_id.reshape(1, rows), member_order.reshape(1, rows),
      cluster_slot.reshape(1, clusters), cluster_size.reshape(1, clusters))
    best, keep, mean = pl.pallas_call(
        finish,
        out_shape=(jax.ShapeDtypeStruct((1, rows), F32), jax.ShapeDtypeStruct((1, rows), I32),
                   jax.ShapeDtypeStruct((1, per_owner), F32)),
        in_specs=[vmem],
        out_specs=(vmem,) * 3,
    )(packed)
    return best.reshape(rows), keep.reshape(rows), mean.reshape(per_owner)


def solution(mesh):
    placed = (P(("rep", "dev"), None), P(("rep", "dev")), P(("rep", "dev")), P("rep"), P("rep"))
    return jax.shard_map(
        body,
        mesh=mesh,
        in_specs=placed,
        out_specs=(P(("rep", "dev")), P(("rep", "dev")), P(("rep", "dev"))),
        check_vma=False,
    )
```

```python
import functools

import jax
import jax.numpy as jnp
from jax import lax
from jax.experimental import pallas as pl
from jax.experimental.pallas import tpu as pltpu
from jax.sharding import PartitionSpec as P

CAP = 128
CHUNK = 128
LOADS = 4
FAR_AHEAD = 4
SLOW = 2
LAG = 2
STRAIGHT = 1
NORM_EPS = 1e-06
CUTOFF = 0.8
META, ORDER, LINE, PLANE, DIRECT, HALF, BACK = range(7)
FIXED = 32000.0
F32 = jnp.float32
BF16 = jnp.bfloat16
I16 = jnp.int16
I32 = jnp.int32


def split_lines(n):
    z = max(z for z in range(1, n + 1) if n % z == 0 and z * z <= n)
    return z, n // z


def source_slots(n, nq, rows, group):
    largest = rows * n // nq + CAP - CAP // nq
    bound = (largest + group * (n - 1)) // n
    return min(group * -(-CAP // n), -(-bound // 16) * 16)


def iota(shape, dim):
    return lax.broadcasted_iota(I32, shape, dim)


def rows_of(values, width):
    row = iota((8, width), 0)
    out = jnp.zeros((8, width), values[0].dtype)
    for r, v in enumerate(values):
        out = jnp.where(row == r, jnp.broadcast_to(v, (8, width)), out)
    return out


def to_col(row, count):
    eye = iota((count, count), 0) == iota((count, count), 1)
    return jnp.sum(jnp.where(eye, row, 0.0), axis=1, keepdims=True)


def floor_div(x, d):
    return jnp.floor((x + 0.5) * (1.0 / d))


def kernel(n, nz, nq, emb_hbm, cid_hbm, order_hbm, slot_hbm, size_hbm, packed_out,
           emb, cid, order, slot, size, unit, line, meta, pick, packed, plane, straight, ots, otr,
           acc, hs, hr, table, units, repack,
           s_load, s_small, r_line, r_plane, sent, came):
    me = lax.axis_index("dev")
    z, q = lax.div(me, nq), lax.rem(me, nq)

    def copy(src, dst, s, r, target):
        return pltpu.make_async_remote_copy(
            src_ref=src, dst_ref=dst, send_sem=s, recv_sem=r,
            device_id={"dev": target}, device_id_type=pl.DeviceIdType.MESH)

    def arrive(ref, sem):
        pltpu.make_async_copy(ref, ref, sem).wait()

    def on_line(d):
        return jnp.bitwise_xor(z, d) * nq + q

    def on_plane(d):
        return z * nq + jnp.bitwise_xor(q, d)

    barrier = pltpu.get_barrier_semaphore()
    friends = [on_line(d) for d in range(1, nz)] + [on_plane(d) for d in range(1, nq)]
    for t in friends:
        pl.semaphore_signal(barrier, inc=1, device_id={"dev": t},
                            device_id_type=pl.DeviceIdType.MESH)
    smalls = [pltpu.make_async_copy(a, b, s_small.at[i]) for i, (a, b) in enumerate(
        [(cid_hbm, cid), (order_hbm, order), (slot_hbm, slot), (size_hbm, size)])]
    parts = s_load.shape[0]
    tall = emb.shape[0] // parts
    loads = [pltpu.make_async_copy(emb_hbm.at[pl.ds(i * tall, tall)], emb.at[pl.ds(i * tall, tall)],
                                   s_load.at[i]) for i in range(parts)]
    for c in smalls + loads:
        c.start()
    rows = emb.shape[0]
    clusters = slot.shape[1]
    per_owner = clusters // n
    chunks, width = line.shape[0], line.shape[3]
    group = nz * per_owner
    per_hub = group // 2
    first_hub = nz // 2 - 1
    slots = plane.shape[2] // nz
    half = CAP // 2
    lined = chunks - STRAIGHT

    for c in smalls:
        c.wait()
    slot_c = to_col(slot[...].astype(F32), clusters)
    size_r = size[...].astype(F32)
    size_c = to_col(size_r, clusters)
    c_row, c_col = iota((clusters, clusters), 1), iota((clusters, clusters), 0)
    ahead = (size_r > size_c) | ((size_r == size_c) & (c_row < c_col))
    place_in = jnp.sum(jnp.where(ahead, 1.0, 0.0), axis=1, keepdims=True)
    e_c = floor_div(place_in, nq)
    turn = place_in - e_c * nq
    odd = e_c - 2.0 * floor_div(e_c, 2)
    g_c = jnp.where(odd > 0.5, nq - 1 - turn, turn)
    hub_c = floor_div(e_c, per_hub)
    work_c = (hub_c * nq + g_c) * per_hub + e_c - hub_c * per_hub
    is_mem = iota((clusters, rows), 0) == cid[...]

    def of_row(v):
        return jnp.sum(jnp.where(is_mem, v, 0.0), axis=0, keepdims=True)

    e_row, work_row = of_row(e_c), of_row(work_c).astype(I32)
    rel = jnp.bitwise_xor(of_row(g_c).astype(I32), q)
    tri = (iota((rows, rows), 0) < iota((rows, rows), 1)).astype(F32).astype(BF16)
    wide_q = -(-nq // 16) * 16
    in_group = iota((wide_q, rows), 0) == rel
    before = jnp.dot(in_group.astype(F32).astype(BF16), tri, preferred_element_type=F32)
    rank = jnp.sum(jnp.where(in_group, before, 0.0), axis=0, keepdims=True)
    place = rel.astype(F32) * slots + rank
    ord_row = order[...].astype(F32)
    meta[0] = rows_of([place, ord_row + 1.0, e_row + 1.0], rows)

    sums = []
    for i in range(parts):
        loads[i].wait()
        x = emb[i * tall:(i + 1) * tall, :]
        sums.append(jnp.sum(x * x, axis=1, keepdims=True))
    scale = lax.rsqrt(jnp.concatenate(sums, axis=0) + NORM_EPS)

    line_order = [d for d in (2, 3, 1) if d < nz] + list(range(4, nz))

    def make_unit(k):
        for t in range(nz):
            c0 = (t * chunks + k) * width
            unit[t, k] = (emb[:, c0:c0 + width] * scale).astype(BF16)

    def send_line(k):
        for d in line_order:
            copy(unit.at[jnp.bitwise_xor(z, d), k], line.at[k, d], sent.at[LINE], r_line.at[k], on_line(d)).start()
        line[k, 0] = unit[z, k]

    pl.semaphore_wait(barrier, len(friends))
    for d in range(1, nz):
        copy(meta.at[0], meta.at[d], sent.at[META], came.at[META], on_line(d)).start()
    far = lax.axis_index("rep") == 0
    for k in range(chunks):
        make_unit(k)
        if k < min(FAR_AHEAD, lined):
            pl.when(far | (k == 0))(functools.partial(send_line, k))
    def label(d):
        pick[d] = jnp.where(iota((nq * slots, rows), 0) == meta[d, 0:1, :].astype(I32), 1.0, 0.0).astype(BF16)
        values = jnp.where((iota((8, rows), 0) == 1) | (iota((8, rows), 0) == 2), meta[d], 0.0).astype(BF16)
        return lax.dot_general(values, pick[d], (((1,), (1,)), ((), ())), preferred_element_type=F32)

    told = [label(0)]
    if STRAIGHT:
        for t in range(nz):
            got = jnp.dot(pick[0], unit[t, chunks - 1], preferred_element_type=F32).astype(BF16)
            straight[t * nq:(t + 1) * nq] = got.reshape(nq, slots, width)
        plane[chunks - 1, 0, 0:slots] = straight[z * nq]
    arrive(meta.at[pl.ds(1, nz - 1)], came.at[META])
    told += [label(d) for d in range(1, nz)]
    for d in range(nq):
        ots[d] = jnp.concatenate([v[:, d * slots:(d + 1) * slots] for v in told], axis=1)
    for d in range(1, nq):
        copy(ots.at[d], otr.at[d], sent.at[ORDER], came.at[ORDER], on_plane(d)).start()

    def make_repack():
        arrive(otr.at[pl.ds(1, nq - 1)], came.at[ORDER])
        labs = jnp.concatenate([ots[0]] + [otr[d] for d in range(1, nq)], axis=1)
        target = ((labs[2:3, :] - 1.0) * CAP + labs[1:2, :] - 1.0).astype(I32)

        def one(e, _):
            hit = iota((CAP, n * slots), 0) + e * CAP == target
            repack[e] = jnp.where(hit, 1.0, 0.0).astype(BF16)
            return 0

        lax.fori_loop(0, group, one, 0)

    pair = 2 if chunks % 2 == 0 else 1
    spans = chunks // pair
    below = iota((half, CAP), 0) + half > iota((half, CAP), 1)
    acc[...] = jnp.zeros(acc.shape, F32)

    def take_line(k):
        arrive(line.at[k, pl.ds(1, nz - 1)], r_line.at[k])

        @pl.when(jnp.logical_not(far) & (k == SLOW) & (k + 1 < lined))
        def _():
            send_line(k + 1)

        ahead = jnp.where(far, FAR_AHEAD, jnp.where(k < SLOW, 1, 2))

        @pl.when(k + ahead < lined)
        def _():
            send_line(k + ahead)

        if STRAIGHT:
            @pl.when(k == max(lined - 3, 0))
            def _():
                for d in range(1, n):
                    dz, dq = divmod(d, nq)
                    copy(straight.at[jnp.bitwise_xor(z, dz) * nq + dq],
                         plane.at[chunks - 1, dq, pl.ds(dz * slots, slots)],
                         sent.at[DIRECT], came.at[DIRECT], jnp.bitwise_xor(z, dz) * nq + jnp.bitwise_xor(q, dq)).start()

        for d in range(nz):
            got = jnp.dot(pick[d], line[k, d], preferred_element_type=F32).astype(BF16)
            plane[k, 0, d * slots:(d + 1) * slots] = got[:slots]
            packed[k, :, d * slots:(d + 1) * slots] = got[slots:].reshape(nq - 1, slots, width)
        for d in range(nq - 1, 0, -1):
            copy(packed.at[k, d - 1], plane.at[k, d], sent.at[PLANE], r_plane.at[k], on_plane(d)).start()

    def take_span(j):
        for i in range(pair):
            k = j * pair + i

            @pl.when(k < lined)
            def _():
                arrive(plane.at[k, pl.ds(1, nq - 1)], r_plane.at[k])

            if STRAIGHT:
                @pl.when(k == lined)
                def _():
                    arrive(straight.at[pl.ds(1, n - 1)], came.at[DIRECT])
        block = [plane[j * pair + i].reshape(n * slots, width) for i in range(pair)]
        block = jnp.concatenate(block, axis=1) if pair > 1 else block[0]
        got = jnp.dot(repack[...].reshape(group * CAP, n * slots), block, preferred_element_type=F32)
        units[...] = got.astype(BF16).reshape(units.shape)

        for b in range(group // 2):
            m = units[b]
            s = lax.dot_general(m, m, (((1,), (1,)), ((), ())), preferred_element_type=F32)
            for l in range(2):
                full = s[l * CAP:(l + 1) * CAP, l * CAP:(l + 1) * CAP]
                part = acc[2 * b + l] + jnp.where(below, full[half:, :], pltpu.roll(full[:half, :], half, 1))
                acc[2 * b + l] = part
                hs[2 * b + l] = jnp.round(part * FIXED).astype(I32).astype(I16)

        @pl.when(j == spans - 1)
        def _():
            for i in range(2):
                h = jnp.where(z > first_hub, i, 1 - i)

                @pl.when(z != first_hub + h)
                def _():
                    copy(hs.at[pl.ds(h * per_hub, per_hub)], hr.at[jnp.bitwise_xor(z, first_hub + h)],
                         sent.at[HALF], came.at[HALF], (first_hub + h) * nq + q).start()

    def step(k, _):
        @pl.when(k < lined)
        def _():
            take_line(k)

        @pl.when(k == min(lined, pair + LAG - 1) - 1)
        def _():
            make_repack()

        back = k - LAG - (pair - 1)

        @pl.when((back >= 0) & (lax.rem(back, pair) == 0))
        def _():
            take_span(lax.div(back, pair))
        return 0

    lax.fori_loop(0, pair * spans + LAG, step, 0)
    arrive(meta.at[pl.ds(1, nz - 1)], sent.at[META])
    arrive(ots.at[pl.ds(1, nq - 1)], sent.at[ORDER])
    arrive(line.at[pl.ds(0, lined), pl.ds(1, nz - 1)], sent.at[LINE])
    arrive(packed.at[pl.ds(0, lined)], sent.at[PLANE])
    if STRAIGHT:
        arrive(straight.at[pl.ds(1, n - 1)], sent.at[DIRECT])

    lane = iota((1, CAP), 1)
    at = jnp.where(lane < half, lane + half, lane - half).astype(F32)
    up_row = iota((half, CAP), 0)
    up_col = iota((half, CAP), 1)
    is_hub = (z == first_hub) | (z == first_hub + 1)
    hub = (z - first_hub) * nq + q

    @pl.when(is_hub)
    def _():
        own = (z - first_hub) * per_hub
        n_mem = []
        for l in range(per_hub):
            w = (hub * per_hub + l).astype(F32)
            n_mem.append(jnp.sum(jnp.where(work_c == w, size_c, 0.0), axis=0, keepdims=True))
        arrive(hr.at[pl.ds(1, nz - 1)], came.at[HALF])
        for l in range(per_hub):
            apart = hr[1, l].astype(I32)
            for d in range(2, nz):
                apart = apart + hr[d, l].astype(I32)
            p = acc[own + l] + apart.astype(F32) * (1.0 / FIXED)
            low = jnp.max(jnp.where(below & (up_col.astype(F32) < n_mem[l]), p, -1.0), axis=1, keepdims=True)
            low = jnp.max(jnp.where(up_row == up_col, low, -1.0), axis=0, keepdims=True)
            top_ok = (up_row + half < up_col) & (up_row.astype(F32) < n_mem[l])
            top = jnp.max(jnp.where(top_ok, p, -1.0), axis=0, keepdims=True)
            live = at < n_mem[l]
            near = jnp.where(live, jnp.where(lane < half, low, top), -1.0)
            mean = jnp.sum(jnp.where(live, near, 0.0), axis=1, keepdims=True) / n_mem[l]
            table[hub, l:l + 1] = jnp.where(lane == half, mean, near)
        for d in range(n - 1, 0, -1):
            copy(table.at[hub], table.at[hub], sent.at[BACK], came.at[BACK], jnp.bitwise_xor(me, d)).start()

    pos = order[...]
    pos = jnp.where(pos < half, pos + half, pos - half)
    hot = jnp.where(iota((clusters, rows), 0) == work_row, 1.0, 0.0)
    hubs = table.shape[0]

    @pl.when(is_hub)
    def _():
        arrive(hs.at[pl.ds(0, per_hub)], sent.at[HALF])
        arrive(table.at[pl.ds(0, hubs - 1)], came.at[BACK])

    @pl.when(jnp.logical_not(is_hub))
    def _():
        arrive(hs, sent.at[HALF])
        arrive(table, came.at[BACK])

    flat = table[...].reshape(clusters, CAP)
    mean = jnp.zeros((1, rows), F32)
    for l in range(per_owner):
        work = jnp.sum(jnp.where(slot_c == (me * per_owner + l).astype(F32), work_c, 0.0), axis=0, keepdims=True).astype(I32)
        hit = (iota((clusters, CAP), 0) == work) & (iota((clusters, CAP), 1) == half)
        part = jnp.sum(jnp.where(hit, flat, 0.0), axis=1, keepdims=True)
        mean = jnp.where(iota((1, rows), 1) == l, jnp.sum(part, axis=0, keepdims=True), mean)
    got = jnp.dot(flat.T, hot, preferred_element_type=F32, precision=lax.Precision.HIGHEST)
    out = jnp.sum(jnp.where(iota((CAP, rows), 0) == pos, got, 0.0), axis=0, keepdims=True)
    out = jnp.where(order[...] == 0, -1.0, out)
    packed_out[...] = rows_of([out, mean], rows)
    @pl.when(is_hub)
    def _():
        for d in range(0, n - 1, hubs - 1):
            arrive(table.at[pl.ds(0, min(hubs - 1, n - 1 - d))], sent.at[BACK])


def finish(packed, best_out, keep_out, mean_out):
    best = packed[0:1, :]
    best_out[...] = best
    keep_out[...] = jnp.where(best < CUTOFF, 1, 0)
    mean_out[...] = packed[1:2, :mean_out.shape[1]]


def body(embeddings, cluster_id, member_order, cluster_slot, cluster_size):
    n = lax.axis_size("dev")
    nz, nq = split_lines(n)
    rows, depth = embeddings.shape
    clusters = cluster_slot.shape[0]
    per_owner = clusters // n
    width = min(CHUNK, depth // nz)
    chunks = depth // nz // width
    group = nz * per_owner
    slots = source_slots(n, nq, rows, group)
    pair = 2 if chunks % 2 == 0 else 1
    half = CAP // 2
    vmem = pl.BlockSpec(memory_space=pltpu.VMEM)
    dma = pltpu.SemaphoreType.DMA
    packed = pl.pallas_call(
        functools.partial(kernel, n, nz, nq),
        out_shape=pltpu.VMEM((8, rows), F32),
        in_specs=[pl.BlockSpec(memory_space=pl.ANY)] * 5,
        out_specs=vmem,
        scratch_shapes=[
            pltpu.VMEM((rows, depth), F32),
            pltpu.VMEM((1, rows), I32),
            pltpu.VMEM((1, rows), I32),
            pltpu.VMEM((1, clusters), I32),
            pltpu.VMEM((1, clusters), I32),
            pltpu.VMEM((nz, chunks, rows, width), BF16),
            pltpu.VMEM((chunks, nz, rows, width), BF16),
            pltpu.VMEM((nz, 8, rows), F32),
            pltpu.VMEM((nz, nq * slots, rows), BF16),
            pltpu.VMEM((chunks, nq - 1, nz * slots, width), BF16),
            pltpu.VMEM((chunks, nq, nz * slots, width), BF16),
            pltpu.VMEM((n, slots, width), BF16),
            pltpu.VMEM((nq, 8, nz * slots), F32),
            pltpu.VMEM((nq, 8, nz * slots), F32),
            pltpu.VMEM((group, half, CAP), F32),
            pltpu.VMEM((group, half, CAP), I16),
            pltpu.VMEM((nz, group // 2, half, CAP), I16),
            pltpu.VMEM((2 * nq, group // 2, CAP), F32),
            pltpu.VMEM((group // 2, 2 * CAP, pair * width), BF16),
            pltpu.VMEM((group, CAP, n * slots), BF16),
            dma((LOADS,)), dma((4,)), dma((chunks,)), dma((chunks,)), dma((7,)), dma((7,)),
        ],
        compiler_params=pltpu.CompilerParams(
            collective_id=0, has_side_effects=True, vmem_limit_bytes=62 * 1024 * 1024),
    )(embeddings, cluster_id.reshape(1, rows), member_order.reshape(1, rows),
      cluster_slot.reshape(1, clusters), cluster_size.reshape(1, clusters))
    best, keep, mean = pl.pallas_call(
        finish,
        out_shape=(jax.ShapeDtypeStruct((1, rows), F32), jax.ShapeDtypeStruct((1, rows), I32),
                   jax.ShapeDtypeStruct((1, per_owner), F32)),
        in_specs=[vmem],
        out_specs=(vmem,) * 3,
    )(pltpu.with_memory_space_constraint(packed, pltpu.VMEM))
    return best.reshape(rows), keep.reshape(rows), mean.reshape(per_owner)


def solution(mesh):
    placed = (P(("rep", "dev"), None), P(("rep", "dev")), P(("rep", "dev")), P("rep"), P("rep"))
    return jax.shard_map(
        body,
        mesh=mesh,
        in_specs=placed,
        out_specs=(P(("rep", "dev")), P(("rep", "dev")), P(("rep", "dev"))),
        check_vma=False,
    )
```

```python
import functools

import jax
import jax.numpy as jnp
from jax import lax
from jax.experimental import pallas as pl
from jax.experimental.pallas import tpu as pltpu
from jax.sharding import PartitionSpec as P

CAP = 128
CHUNK = 128
LOADS = 4
FAR_AHEAD = 4
SLOW = 2
LAG = 2
STRAIGHT = 1
NORM_EPS = 1e-06
CUTOFF = 0.8
META, ORDER, LINE, PLANE, DIRECT, HALF, BACK = range(7)
FIXED = 32000.0
F32 = jnp.float32
BF16 = jnp.bfloat16
I16 = jnp.int16
I32 = jnp.int32


def split_lines(n):
    z = max(z for z in range(1, n + 1) if n % z == 0 and z * z <= n)
    return z, n // z


def source_slots(n, nq, rows, group):
    largest = rows * n // nq + CAP - CAP // nq
    bound = (largest + group * (n - 1)) // n
    return min(group * -(-CAP // n), -(-bound // 16) * 16)


def iota(shape, dim):
    return lax.broadcasted_iota(I32, shape, dim)


def rows_of(values, width):
    row = iota((8, width), 0)
    out = jnp.zeros((8, width), values[0].dtype)
    for r, v in enumerate(values):
        out = jnp.where(row == r, jnp.broadcast_to(v, (8, width)), out)
    return out


def to_col(row, count):
    eye = iota((count, count), 0) == iota((count, count), 1)
    return jnp.sum(jnp.where(eye, row, 0.0), axis=1, keepdims=True)


def floor_div(x, d):
    return jnp.floor((x + 0.5) * (1.0 / d))


def kernel(n, nz, nq, emb_hbm, cid_hbm, order_hbm, slot_hbm, size_hbm, packed_out,
           emb, cid, order, slot, size, unit, line, meta, pick, packed, plane, straight, ots, otr,
           acc, hs, hr, table, units, repack,
           s_load, s_small, r_line, r_plane, sent, came):
    me = lax.axis_index("dev")
    z, q = lax.div(me, nq), lax.rem(me, nq)

    def copy(src, dst, s, r, target):
        return pltpu.make_async_remote_copy(
            src_ref=src, dst_ref=dst, send_sem=s, recv_sem=r,
            device_id={"dev": target}, device_id_type=pl.DeviceIdType.MESH)

    def arrive(ref, sem):
        pltpu.make_async_copy(ref, ref, sem).wait()

    def on_line(d):
        return jnp.bitwise_xor(z, d) * nq + q

    def on_plane(d):
        return z * nq + jnp.bitwise_xor(q, d)

    barrier = pltpu.get_barrier_semaphore()
    friends = [on_line(d) for d in range(1, nz)] + [on_plane(d) for d in range(1, nq)]
    for t in friends:
        pl.semaphore_signal(barrier, inc=1, device_id={"dev": t},
                            device_id_type=pl.DeviceIdType.MESH)
    smalls = [pltpu.make_async_copy(a, b, s_small.at[i]) for i, (a, b) in enumerate(
        [(cid_hbm, cid), (order_hbm, order), (slot_hbm, slot), (size_hbm, size)])]
    parts = s_load.shape[0]
    tall = emb.shape[0] // parts
    loads = [pltpu.make_async_copy(emb_hbm.at[pl.ds(i * tall, tall)], emb.at[pl.ds(i * tall, tall)],
                                   s_load.at[i]) for i in range(parts)]
    for c in smalls + loads:
        c.start()
    rows = emb.shape[0]
    clusters = slot.shape[1]
    per_owner = clusters // n
    chunks, width = line.shape[0], line.shape[3]
    group = nz * per_owner
    per_hub = group // 2
    first_hub = nz // 2 - 1
    slots = plane.shape[2] // nz
    half = CAP // 2
    lined = chunks - STRAIGHT

    for c in smalls:
        c.wait()
    slot_c = to_col(slot[...].astype(F32), clusters)
    size_r = size[...].astype(F32)
    size_c = to_col(size_r, clusters)
    c_row, c_col = iota((clusters, clusters), 1), iota((clusters, clusters), 0)
    ahead = (size_r > size_c) | ((size_r == size_c) & (c_row < c_col))
    place_in = jnp.sum(jnp.where(ahead, 1.0, 0.0), axis=1, keepdims=True)
    e_c = floor_div(place_in, nq)
    turn = place_in - e_c * nq
    odd = e_c - 2.0 * floor_div(e_c, 2)
    g_c = jnp.where(odd > 0.5, nq - 1 - turn, turn)
    hub_c = floor_div(e_c, per_hub)
    work_c = (hub_c * nq + g_c) * per_hub + e_c - hub_c * per_hub
    is_mem = iota((clusters, rows), 0) == cid[...]

    def of_row(v):
        return jnp.sum(jnp.where(is_mem, v, 0.0), axis=0, keepdims=True)

    e_row, work_row = of_row(e_c), of_row(work_c).astype(I32)
    rel = jnp.bitwise_xor(of_row(g_c).astype(I32), q)
    tri = (iota((rows, rows), 0) < iota((rows, rows), 1)).astype(F32).astype(BF16)
    wide_q = -(-nq // 16) * 16
    in_group = iota((wide_q, rows), 0) == rel
    before = jnp.dot(in_group.astype(F32).astype(BF16), tri, preferred_element_type=F32)
    rank = jnp.sum(jnp.where(in_group, before, 0.0), axis=0, keepdims=True)
    place = rel.astype(F32) * slots + rank
    ord_row = order[...].astype(F32)
    meta[0] = rows_of([place, ord_row + 1.0, e_row + 1.0], rows)

    sums = []
    for i in range(parts):
        loads[i].wait()
        x = emb[i * tall:(i + 1) * tall, :]
        sums.append(jnp.sum(x * x, axis=1, keepdims=True))
    scale = lax.rsqrt(jnp.concatenate(sums, axis=0) + NORM_EPS)

    line_order = [d for d in (3, 2, 1) if d < nz] + list(range(4, nz))

    def make_unit(k):
        for t in range(nz):
            c0 = (t * chunks + k) * width
            unit[t, k] = (emb[:, c0:c0 + width] * scale).astype(BF16)

    def send_line(k):
        for d in line_order:
            copy(unit.at[jnp.bitwise_xor(z, d), k], line.at[k, d], sent.at[LINE], r_line.at[k], on_line(d)).start()
        line[k, 0] = unit[z, k]

    pl.semaphore_wait(barrier, len(friends))
    for d in range(1, nz):
        copy(meta.at[0], meta.at[d], sent.at[META], came.at[META], on_line(d)).start()
    far = lax.axis_index("rep") == 0
    for k in range(chunks):
        make_unit(k)
        if k < min(FAR_AHEAD, lined):
            pl.when(far | (k == 0))(functools.partial(send_line, k))
    def label(d):
        pick[d] = jnp.where(iota((nq * slots, rows), 0) == meta[d, 0:1, :].astype(I32), 1.0, 0.0).astype(BF16)
        values = jnp.where((iota((8, rows), 0) == 1) | (iota((8, rows), 0) == 2), meta[d], 0.0).astype(BF16)
        return lax.dot_general(values, pick[d], (((1,), (1,)), ((), ())), preferred_element_type=F32)

    told = [label(0)]
    if STRAIGHT:
        for t in range(nz):
            got = jnp.dot(pick[0], unit[t, chunks - 1], preferred_element_type=F32).astype(BF16)
            straight[t * nq:(t + 1) * nq] = got.reshape(nq, slots, width)
        plane[chunks - 1, 0, 0:slots] = straight[z * nq]
    arrive(meta.at[pl.ds(1, nz - 1)], came.at[META])
    told += [label(d) for d in range(1, nz)]
    for d in range(nq):
        ots[d] = jnp.concatenate([v[:, d * slots:(d + 1) * slots] for v in told], axis=1)
    for d in range(1, nq):
        copy(ots.at[d], otr.at[d], sent.at[ORDER], came.at[ORDER], on_plane(d)).start()

    def make_repack():
        arrive(otr.at[pl.ds(1, nq - 1)], came.at[ORDER])
        labs = jnp.concatenate([ots[0]] + [otr[d] for d in range(1, nq)], axis=1)
        target = ((labs[2:3, :] - 1.0) * CAP + labs[1:2, :] - 1.0).astype(I32)

        def one(e, _):
            hit = iota((CAP, n * slots), 0) + e * CAP == target
            repack[e] = jnp.where(hit, 1.0, 0.0).astype(BF16)
            return 0

        lax.fori_loop(0, group, one, 0)

    pair = 2 if chunks % 2 == 0 else 1
    spans = chunks // pair
    below = iota((half, CAP), 0) + half > iota((half, CAP), 1)
    acc[...] = jnp.zeros(acc.shape, F32)

    def take_line(k):
        arrive(line.at[k, pl.ds(1, nz - 1)], r_line.at[k])

        @pl.when(jnp.logical_not(far) & (k == SLOW) & (k + 1 < lined))
        def _():
            send_line(k + 1)

        ahead = jnp.where(far, FAR_AHEAD, jnp.where(k < SLOW, 1, 2))

        @pl.when(k + ahead < lined)
        def _():
            send_line(k + ahead)

        if STRAIGHT:
            @pl.when(k == max(lined - 3, 0))
            def _():
                for d in range(1, n):
                    dz, dq = divmod(d, nq)
                    copy(straight.at[jnp.bitwise_xor(z, dz) * nq + dq],
                         plane.at[chunks - 1, dq, pl.ds(dz * slots, slots)],
                         sent.at[DIRECT], came.at[DIRECT], jnp.bitwise_xor(z, dz) * nq + jnp.bitwise_xor(q, dq)).start()

        for d in range(nz):
            got = jnp.dot(pick[d], line[k, d], preferred_element_type=F32).astype(BF16)
            plane[k, 0, d * slots:(d + 1) * slots] = got[:slots]
            packed[k, :, d * slots:(d + 1) * slots] = got[slots:].reshape(nq - 1, slots, width)
        for d in range(nq - 1, 0, -1):
            copy(packed.at[k, d - 1], plane.at[k, d], sent.at[PLANE], r_plane.at[k], on_plane(d)).start()

    def take_span(j):
        for i in range(pair):
            k = j * pair + i

            @pl.when(k < lined)
            def _():
                arrive(plane.at[k, pl.ds(1, nq - 1)], r_plane.at[k])

            if STRAIGHT:
                @pl.when(k == lined)
                def _():
                    arrive(straight.at[pl.ds(1, n - 1)], came.at[DIRECT])
        block = [plane[j * pair + i].reshape(n * slots, width) for i in range(pair)]
        block = jnp.concatenate(block, axis=1) if pair > 1 else block[0]
        got = jnp.dot(repack[...].reshape(group * CAP, n * slots), block, preferred_element_type=F32)
        units[...] = got.astype(BF16).reshape(units.shape)

        for i in range(2):
            h = jnp.where(z > first_hub, i, 1 - i)
            for e in range(0, per_hub, 2):
                e = h * per_hub + e
                m = units[lax.div(e, 2)]
                s = lax.dot_general(m, m, (((1,), (1,)), ((), ())), preferred_element_type=F32)
                for l in range(2):
                    full = s[l * CAP:(l + 1) * CAP, l * CAP:(l + 1) * CAP]
                    part = acc[e + l] + jnp.where(below, full[half:, :], pltpu.roll(full[:half, :], half, 1))
                    acc[e + l] = part
                    hs[e + l] = jnp.round(part * FIXED).astype(I32).astype(I16)

            @pl.when((j == spans - 1) & (z != first_hub + h))
            def _():
                copy(hs.at[pl.ds(h * per_hub, per_hub)], hr.at[jnp.bitwise_xor(z, first_hub + h)],
                     sent.at[HALF], came.at[HALF], (first_hub + h) * nq + q).start()

    def step(k, _):
        @pl.when(k < lined)
        def _():
            take_line(k)

        @pl.when(k == min(lined, pair + LAG - 1) - 1)
        def _():
            make_repack()

        back = k - LAG - (pair - 1)

        @pl.when((back >= 0) & (lax.rem(back, pair) == 0))
        def _():
            take_span(lax.div(back, pair))
        return 0

    lax.fori_loop(0, pair * spans + LAG, step, 0)
    arrive(meta.at[pl.ds(1, nz - 1)], sent.at[META])
    arrive(ots.at[pl.ds(1, nq - 1)], sent.at[ORDER])
    arrive(line.at[pl.ds(0, lined), pl.ds(1, nz - 1)], sent.at[LINE])
    arrive(packed.at[pl.ds(0, lined)], sent.at[PLANE])
    if STRAIGHT:
        arrive(straight.at[pl.ds(1, n - 1)], sent.at[DIRECT])

    lane = iota((1, CAP), 1)
    at = jnp.where(lane < half, lane + half, lane - half).astype(F32)
    up_row = iota((half, CAP), 0)
    up_col = iota((half, CAP), 1)
    is_hub = (z == first_hub) | (z == first_hub + 1)
    hub = (z - first_hub) * nq + q

    @pl.when(is_hub)
    def _():
        own = (z - first_hub) * per_hub
        n_mem = []
        for l in range(per_hub):
            w = (hub * per_hub + l).astype(F32)
            n_mem.append(jnp.sum(jnp.where(work_c == w, size_c, 0.0), axis=0, keepdims=True))
        arrive(hr.at[pl.ds(1, nz - 1)], came.at[HALF])
        for l in range(per_hub):
            apart = hr[1, l].astype(I32)
            for d in range(2, nz):
                apart = apart + hr[d, l].astype(I32)
            p = acc[own + l] + apart.astype(F32) * (1.0 / FIXED)
            low = jnp.max(jnp.where(below & (up_col.astype(F32) < n_mem[l]), p, -1.0), axis=1, keepdims=True)
            low = jnp.max(jnp.where(up_row == up_col, low, -1.0), axis=0, keepdims=True)
            top_ok = (up_row + half < up_col) & (up_row.astype(F32) < n_mem[l])
            top = jnp.max(jnp.where(top_ok, p, -1.0), axis=0, keepdims=True)
            live = at < n_mem[l]
            near = jnp.where(live, jnp.where(lane < half, low, top), -1.0)
            mean = jnp.sum(jnp.where(live, near, 0.0), axis=1, keepdims=True) / n_mem[l]
            table[hub, l:l + 1] = jnp.where(lane == half, mean, near)
        for d in sorted(range(1, n), key=lambda d: d // nq in (0, nz - 1)):
            copy(table.at[hub], table.at[hub], sent.at[BACK], came.at[BACK], jnp.bitwise_xor(me, d)).start()

    pos = order[...]
    pos = jnp.where(pos < half, pos + half, pos - half)
    hot = jnp.where(iota((clusters, rows), 0) == work_row, 1.0, 0.0)
    hubs = table.shape[0]

    @pl.when(is_hub)
    def _():
        arrive(hs.at[pl.ds(0, per_hub)], sent.at[HALF])
        arrive(table.at[pl.ds(0, hubs - 1)], came.at[BACK])

    @pl.when(jnp.logical_not(is_hub))
    def _():
        arrive(hs, sent.at[HALF])
        arrive(table, came.at[BACK])

    flat = table[...].reshape(clusters, CAP)
    mean = jnp.zeros((1, rows), F32)
    for l in range(per_owner):
        work = jnp.sum(jnp.where(slot_c == (me * per_owner + l).astype(F32), work_c, 0.0), axis=0, keepdims=True).astype(I32)
        hit = (iota((clusters, CAP), 0) == work) & (iota((clusters, CAP), 1) == half)
        part = jnp.sum(jnp.where(hit, flat, 0.0), axis=1, keepdims=True)
        mean = jnp.where(iota((1, rows), 1) == l, jnp.sum(part, axis=0, keepdims=True), mean)
    got = jnp.dot(flat.T, hot, preferred_element_type=F32, precision=lax.Precision.HIGHEST)
    out = jnp.sum(jnp.where(iota((CAP, rows), 0) == pos, got, 0.0), axis=0, keepdims=True)
    out = jnp.where(order[...] == 0, -1.0, out)
    packed_out[...] = rows_of([out, mean], rows)
    @pl.when(is_hub)
    def _():
        for d in range(0, n - 1, hubs - 1):
            arrive(table.at[pl.ds(0, min(hubs - 1, n - 1 - d))], sent.at[BACK])


def finish(packed, best_out, keep_out, mean_out):
    best = packed[0:1, :]
    best_out[...] = best
    keep_out[...] = jnp.where(best < CUTOFF, 1, 0)
    mean_out[...] = packed[1:2, :mean_out.shape[1]]


def body(embeddings, cluster_id, member_order, cluster_slot, cluster_size):
    n = lax.axis_size("dev")
    nz, nq = split_lines(n)
    rows, depth = embeddings.shape
    clusters = cluster_slot.shape[0]
    per_owner = clusters // n
    width = min(CHUNK, depth // nz)
    chunks = depth // nz // width
    group = nz * per_owner
    slots = source_slots(n, nq, rows, group)
    pair = 2 if chunks % 2 == 0 else 1
    half = CAP // 2
    vmem = pl.BlockSpec(memory_space=pltpu.VMEM)
    dma = pltpu.SemaphoreType.DMA
    packed = pl.pallas_call(
        functools.partial(kernel, n, nz, nq),
        out_shape=pltpu.VMEM((8, rows), F32),
        in_specs=[pl.BlockSpec(memory_space=pl.ANY)] * 5,
        out_specs=vmem,
        scratch_shapes=[
            pltpu.VMEM((rows, depth), F32),
            pltpu.VMEM((1, rows), I32),
            pltpu.VMEM((1, rows), I32),
            pltpu.VMEM((1, clusters), I32),
            pltpu.VMEM((1, clusters), I32),
            pltpu.VMEM((nz, chunks, rows, width), BF16),
            pltpu.VMEM((chunks, nz, rows, width), BF16),
            pltpu.VMEM((nz, 8, rows), F32),
            pltpu.VMEM((nz, nq * slots, rows), BF16),
            pltpu.VMEM((chunks, nq - 1, nz * slots, width), BF16),
            pltpu.VMEM((chunks, nq, nz * slots, width), BF16),
            pltpu.VMEM((n, slots, width), BF16),
            pltpu.VMEM((nq, 8, nz * slots), F32),
            pltpu.VMEM((nq, 8, nz * slots), F32),
            pltpu.VMEM((group, half, CAP), F32),
            pltpu.VMEM((group, half, CAP), I16),
            pltpu.VMEM((nz, group // 2, half, CAP), I16),
            pltpu.VMEM((2 * nq, group // 2, CAP), F32),
            pltpu.VMEM((group // 2, 2 * CAP, pair * width), BF16),
            pltpu.VMEM((group, CAP, n * slots), BF16),
            dma((LOADS,)), dma((4,)), dma((chunks,)), dma((chunks,)), dma((7,)), dma((7,)),
        ],
        compiler_params=pltpu.CompilerParams(
            collective_id=0, has_side_effects=True, vmem_limit_bytes=62 * 1024 * 1024),
    )(embeddings, cluster_id.reshape(1, rows), member_order.reshape(1, rows),
      cluster_slot.reshape(1, clusters), cluster_size.reshape(1, clusters))
    best, keep, mean = pl.pallas_call(
        finish,
        out_shape=(jax.ShapeDtypeStruct((1, rows), F32), jax.ShapeDtypeStruct((1, rows), I32),
                   jax.ShapeDtypeStruct((1, per_owner), F32)),
        in_specs=[vmem],
        out_specs=(vmem,) * 3,
    )(pltpu.with_memory_space_constraint(packed, pltpu.VMEM))
    return best.reshape(rows), keep.reshape(rows), mean.reshape(per_owner)


def solution(mesh):
    placed = (P(("rep", "dev"), None), P(("rep", "dev")), P(("rep", "dev")), P("rep"), P("rep"))
    return jax.shard_map(
        body,
        mesh=mesh,
        in_specs=placed,
        out_specs=(P(("rep", "dev")), P(("rep", "dev")), P(("rep", "dev"))),
        check_vma=False,
    )
```

```python
import functools

import jax
import jax.numpy as jnp
from jax import lax
from jax.experimental import pallas as pl
from jax.experimental.pallas import tpu as pltpu
from jax.sharding import PartitionSpec as P

CAP = 128
CHUNK = 128
LOADS = 4
FAR_AHEAD = 4
SLOW = 2
LAG = 2
STRAIGHT = 1
NORM_EPS = 1e-06
CUTOFF = 0.8
META, ORDER, DIRECT, HALF, BACK, LINE, PLANE = range(7)
FIXED = 32000.0
F32 = jnp.float32
BF16 = jnp.bfloat16
I16 = jnp.int16
I32 = jnp.int32


def split_lines(n):
    z = max(z for z in range(1, n + 1) if n % z == 0 and z * z <= n)
    return z, n // z


def source_slots(n, nq, rows, group):
    largest = rows * n // nq + CAP - CAP // nq
    bound = (largest + group * (n - 1)) // n
    return min(group * -(-CAP // n), -(-bound // 16) * 16)


def iota(shape, dim):
    return lax.broadcasted_iota(I32, shape, dim)


def rows_of(values, width):
    row = iota((8, width), 0)
    out = jnp.zeros((8, width), values[0].dtype)
    for r, v in enumerate(values):
        out = jnp.where(row == r, jnp.broadcast_to(v, (8, width)), out)
    return out


def to_col(row, count):
    eye = iota((count, count), 0) == iota((count, count), 1)
    return jnp.sum(jnp.where(eye, row, 0.0), axis=1, keepdims=True)


def floor_div(x, d):
    return jnp.floor((x + 0.5) * (1.0 / d))


def kernel(n, nz, nq, emb_hbm, cid_hbm, order_hbm, slot_hbm, size_hbm, packed_out,
           emb, cid, order, slot, size, unit, line, meta, pick, packed, plane, straight, ots, otr,
           acc, hs, hr, table, units, repack,
           s_load, s_small, r_line, r_plane, sent, came):
    me = lax.axis_index("dev")
    z, q = lax.div(me, nq), lax.rem(me, nq)

    def copy(src, dst, s, r, target):
        return pltpu.make_async_remote_copy(
            src_ref=src, dst_ref=dst, send_sem=s, recv_sem=r,
            device_id={"dev": target}, device_id_type=pl.DeviceIdType.MESH)

    def arrive(ref, sem):
        pltpu.make_async_copy(ref, ref, sem).wait()

    def on_line(d):
        return jnp.bitwise_xor(z, d) * nq + q

    def on_plane(d):
        return z * nq + jnp.bitwise_xor(q, d)

    barrier = pltpu.get_barrier_semaphore()
    friends = [on_line(d) for d in range(1, nz)] + [on_plane(d) for d in range(1, nq)]
    for t in friends:
        pl.semaphore_signal(barrier, inc=1, device_id={"dev": t},
                            device_id_type=pl.DeviceIdType.MESH)
    smalls = [pltpu.make_async_copy(a, b, s_small.at[i]) for i, (a, b) in enumerate(
        [(cid_hbm, cid), (order_hbm, order), (slot_hbm, slot), (size_hbm, size)])]
    parts = s_load.shape[0]
    tall = emb.shape[0] // parts
    loads = [pltpu.make_async_copy(emb_hbm.at[pl.ds(i * tall, tall)], emb.at[pl.ds(i * tall, tall)],
                                   s_load.at[i]) for i in range(parts)]
    for c in smalls + loads:
        c.start()
    rows = emb.shape[0]
    clusters = slot.shape[1]
    per_owner = clusters // n
    chunks, width = line.shape[0], line.shape[3]
    group = nz * per_owner
    per_hub = group // 2
    first_hub = nz // 2 - 1
    slots = plane.shape[2] // nz
    half = CAP // 2
    lined = chunks - STRAIGHT

    for c in smalls:
        c.wait()
    slot_c = to_col(slot[...].astype(F32), clusters)
    size_r = size[...].astype(F32)
    size_c = to_col(size_r, clusters)
    c_row, c_col = iota((clusters, clusters), 1), iota((clusters, clusters), 0)
    ahead = (size_r > size_c) | ((size_r == size_c) & (c_row < c_col))
    place_in = jnp.sum(jnp.where(ahead, 1.0, 0.0), axis=1, keepdims=True)
    e_c = floor_div(place_in, nq)
    turn = place_in - e_c * nq
    odd = e_c - 2.0 * floor_div(e_c, 2)
    g_c = jnp.where(odd > 0.5, nq - 1 - turn, turn)
    hub_c = floor_div(e_c, per_hub)
    work_c = (hub_c * nq + g_c) * per_hub + e_c - hub_c * per_hub
    is_mem = iota((clusters, rows), 0) == cid[...]

    def of_row(v):
        return jnp.sum(jnp.where(is_mem, v, 0.0), axis=0, keepdims=True)

    e_row, work_row = of_row(e_c), of_row(work_c).astype(I32)
    rel = jnp.bitwise_xor(of_row(g_c).astype(I32), q)
    tri = (iota((rows, rows), 0) < iota((rows, rows), 1)).astype(F32).astype(BF16)
    wide_q = -(-nq // 16) * 16
    in_group = iota((wide_q, rows), 0) == rel
    before = jnp.dot(in_group.astype(F32).astype(BF16), tri, preferred_element_type=F32)
    rank = jnp.sum(jnp.where(in_group, before, 0.0), axis=0, keepdims=True)
    place = rel.astype(F32) * slots + rank
    ord_row = order[...].astype(F32)
    meta[0] = rows_of([place, ord_row + 1.0, e_row + 1.0], rows)

    sums = []
    for i in range(parts):
        loads[i].wait()
        x = emb[i * tall:(i + 1) * tall, :]
        sums.append(jnp.sum(x * x, axis=1, keepdims=True))
    scale = lax.rsqrt(jnp.concatenate(sums, axis=0) + NORM_EPS)

    line_order = [d for d in (3, 2, 1) if d < nz] + list(range(4, nz))

    def make_unit(k):
        for t in range(nz):
            c0 = (t * chunks + k) * width
            unit[t, k] = (emb[:, c0:c0 + width] * scale).astype(BF16)

    def send_line(k):
        for d in line_order:
            copy(unit.at[jnp.bitwise_xor(z, d), k], line.at[k, d], sent.at[LINE], r_line.at[k], on_line(d)).start()
        line[k, 0] = unit[z, k]

    pl.semaphore_wait(barrier, len(friends))
    for d in range(1, nz):
        copy(meta.at[0], meta.at[d], sent.at[META], came.at[META], on_line(d)).start()
    far = lax.axis_index("rep") == 0
    for k in range(chunks):
        make_unit(k)
        if k < min(FAR_AHEAD, lined):
            pl.when(far | (k == 0))(functools.partial(send_line, k))
    def label(d):
        pick[d] = jnp.where(iota((nq * slots, rows), 0) == meta[d, 0:1, :].astype(I32), 1.0, 0.0).astype(BF16)
        values = jnp.where((iota((8, rows), 0) == 1) | (iota((8, rows), 0) == 2), meta[d], 0.0).astype(BF16)
        return lax.dot_general(values, pick[d], (((1,), (1,)), ((), ())), preferred_element_type=F32)

    told = [label(0)]
    if STRAIGHT:
        for t in range(nz):
            got = jnp.dot(pick[0], unit[t, chunks - 1], preferred_element_type=F32).astype(BF16)
            straight[t * nq:(t + 1) * nq] = got.reshape(nq, slots, width)
        plane[chunks - 1, 0, 0:slots] = straight[z * nq]
    arrive(meta.at[pl.ds(1, nz - 1)], came.at[META])
    told += [label(d) for d in range(1, nz)]
    for d in range(nq):
        ots[d] = jnp.concatenate([v[:, d * slots:(d + 1) * slots] for v in told], axis=1)
    for d in range(1, nq):
        copy(ots.at[d], otr.at[d], sent.at[ORDER], came.at[ORDER], on_plane(d)).start()

    def make_repack():
        arrive(otr.at[pl.ds(1, nq - 1)], came.at[ORDER])
        labs = jnp.concatenate([ots[0]] + [otr[d] for d in range(1, nq)], axis=1)
        target = ((labs[2:3, :] - 1.0) * CAP + labs[1:2, :] - 1.0).astype(I32)

        def one(e, _):
            hit = iota((CAP, n * slots), 0) + e * CAP == target
            repack[e] = jnp.where(hit, 1.0, 0.0).astype(BF16)
            return 0

        lax.fori_loop(0, group, one, 0)

    pair = 2 if chunks % 2 == 0 else 1
    spans = chunks // pair
    below = iota((half, CAP), 0) + half > iota((half, CAP), 1)
    acc[...] = jnp.zeros(acc.shape, F32)

    def take_line(k):
        arrive(line.at[k, pl.ds(1, nz - 1)], r_line.at[k])

        @pl.when(jnp.logical_not(far) & (k == SLOW) & (k + 1 < lined))
        def _():
            send_line(k + 1)

        ahead = jnp.where(far, FAR_AHEAD, jnp.where(k < SLOW, 1, 2))

        @pl.when(k + ahead < lined)
        def _():
            send_line(k + ahead)

        if STRAIGHT:
            @pl.when(k == max(lined - 3, 0))
            def _():
                for d in range(1, n):
                    dz, dq = divmod(d, nq)
                    copy(straight.at[jnp.bitwise_xor(z, dz) * nq + dq],
                         plane.at[chunks - 1, dq, pl.ds(dz * slots, slots)],
                         sent.at[DIRECT], came.at[DIRECT], jnp.bitwise_xor(z, dz) * nq + jnp.bitwise_xor(q, dq)).start()

        for d in range(nz):
            got = jnp.dot(pick[d], line[k, d], preferred_element_type=F32).astype(BF16)
            plane[k, 0, d * slots:(d + 1) * slots] = got[:slots]
            packed[k, :, d * slots:(d + 1) * slots] = got[slots:].reshape(nq - 1, slots, width)
        for d in range(nq - 1, 0, -1):
            copy(packed.at[k, d - 1], plane.at[k, d], sent.at[PLANE], r_plane.at[k], on_plane(d)).start()

    def take_span(j):
        for i in range(pair):
            k = j * pair + i

            @pl.when(k < lined)
            def _():
                arrive(plane.at[k, pl.ds(1, nq - 1)], r_plane.at[k])

            if STRAIGHT:
                @pl.when(k == lined)
                def _():
                    arrive(straight.at[pl.ds(1, n - 1)], came.at[DIRECT])
        block = [plane[j * pair + i].reshape(n * slots, width) for i in range(pair)]
        block = jnp.concatenate(block, axis=1) if pair > 1 else block[0]
        got = jnp.dot(repack[...].reshape(group * CAP, n * slots), block, preferred_element_type=F32)
        units[...] = got.astype(BF16).reshape(units.shape)

        for i in range(2):
            h = jnp.where(z > first_hub, i, 1 - i)
            for e in range(0, per_hub, 2):
                e = h * per_hub + e
                m = units[lax.div(e, 2)]
                s = lax.dot_general(m, m, (((1,), (1,)), ((), ())), preferred_element_type=F32)
                for l in range(2):
                    full = s[l * CAP:(l + 1) * CAP, l * CAP:(l + 1) * CAP]
                    part = acc[e + l] + jnp.where(below, full[half:, :], pltpu.roll(full[:half, :], half, 1))
                    acc[e + l] = part

            @pl.when((j == spans - 1) & (z != first_hub + h))
            def _():
                for l in range(per_hub):
                    hs[h * per_hub + l] = jnp.round(acc[h * per_hub + l] * FIXED).astype(I32).astype(I16)
                copy(hs.at[pl.ds(h * per_hub, per_hub)], hr.at[jnp.bitwise_xor(z, first_hub + h)],
                     sent.at[HALF], came.at[HALF], (first_hub + h) * nq + q).start()

    def step(k, _):
        @pl.when(k < lined)
        def _():
            take_line(k)

        @pl.when(k == min(lined, pair + LAG - 1) - 1)
        def _():
            make_repack()

        back = k - LAG - (pair - 1)

        @pl.when((back >= 0) & (lax.rem(back, pair) == 0))
        def _():
            take_span(lax.div(back, pair))
        return 0

    lax.fori_loop(0, pair * spans + LAG, step, 0)
    arrive(meta.at[pl.ds(1, nz - 1)], sent.at[META])
    arrive(ots.at[pl.ds(1, nq - 1)], sent.at[ORDER])
    arrive(line.at[pl.ds(0, lined), pl.ds(1, nz - 1)], sent.at[LINE])
    arrive(packed.at[pl.ds(0, lined)], sent.at[PLANE])
    if STRAIGHT:
        arrive(straight.at[pl.ds(1, n - 1)], sent.at[DIRECT])

    lane = iota((1, CAP), 1)
    at = jnp.where(lane < half, lane + half, lane - half).astype(F32)
    up_row = iota((half, CAP), 0)
    up_col = iota((half, CAP), 1)
    is_hub = (z == first_hub) | (z == first_hub + 1)
    hub = (z - first_hub) * nq + q

    @pl.when(is_hub)
    def _():
        own = (z - first_hub) * per_hub
        n_mem = []
        for l in range(per_hub):
            w = (hub * per_hub + l).astype(F32)
            n_mem.append(jnp.sum(jnp.where(work_c == w, size_c, 0.0), axis=0, keepdims=True))
        arrive(hr.at[pl.ds(1, nz - 1)], came.at[HALF])
        for l in range(per_hub):
            apart = hr[1, l].astype(I32)
            for d in range(2, nz):
                apart = apart + hr[d, l].astype(I32)
            p = acc[own + l] + apart.astype(F32) * (1.0 / FIXED)
            low = jnp.max(jnp.where(below & (up_col.astype(F32) < n_mem[l]), p, -1.0), axis=1, keepdims=True)
            low = jnp.max(jnp.where(up_row == up_col, low, -1.0), axis=0, keepdims=True)
            top_ok = (up_row + half < up_col) & (up_row.astype(F32) < n_mem[l])
            top = jnp.max(jnp.where(top_ok, p, -1.0), axis=0, keepdims=True)
            live = at < n_mem[l]
            near = jnp.where(live, jnp.where(lane < half, low, top), -1.0)
            mean = jnp.sum(jnp.where(live, near, 0.0), axis=1, keepdims=True) / n_mem[l]
            table[hub, l:l + 1] = jnp.where(lane == half, mean, near)
        for d in sorted(range(1, n), key=lambda d: d // nq in (0, nz - 1)):
            copy(table.at[hub], table.at[hub], sent.at[BACK], came.at[BACK], jnp.bitwise_xor(me, d)).start()

    pos = order[...]
    pos = jnp.where(pos < half, pos + half, pos - half)
    hot = jnp.where(iota((clusters, rows), 0) == work_row, 1.0, 0.0)
    hubs = table.shape[0]

    @pl.when(is_hub)
    def _():
        arrive(hs.at[pl.ds(0, per_hub)], sent.at[HALF])
        arrive(table.at[pl.ds(0, hubs - 1)], came.at[BACK])

    @pl.when(jnp.logical_not(is_hub))
    def _():
        arrive(hs, sent.at[HALF])
        arrive(table, came.at[BACK])

    flat = table[...].reshape(clusters, CAP)
    mean = jnp.zeros((1, rows), F32)
    for l in range(per_owner):
        work = jnp.sum(jnp.where(slot_c == (me * per_owner + l).astype(F32), work_c, 0.0), axis=0, keepdims=True).astype(I32)
        hit = (iota((clusters, CAP), 0) == work) & (iota((clusters, CAP), 1) == half)
        part = jnp.sum(jnp.where(hit, flat, 0.0), axis=1, keepdims=True)
        mean = jnp.where(iota((1, rows), 1) == l, jnp.sum(part, axis=0, keepdims=True), mean)
    got = jnp.dot(flat.T, hot, preferred_element_type=F32, precision=lax.Precision.HIGHEST)
    out = jnp.sum(jnp.where(iota((CAP, rows), 0) == pos, got, 0.0), axis=0, keepdims=True)
    out = jnp.where(order[...] == 0, -1.0, out)
    packed_out[...] = rows_of([out, mean], rows)
    @pl.when(is_hub)
    def _():
        for d in range(0, n - 1, hubs - 1):
            arrive(table.at[pl.ds(0, min(hubs - 1, n - 1 - d))], sent.at[BACK])


def finish(packed, best_out, keep_out, mean_out):
    best = packed[0:1, :]
    best_out[...] = best
    keep_out[...] = jnp.where(best < CUTOFF, 1, 0)
    mean_out[...] = packed[1:2, :mean_out.shape[1]]


def body(embeddings, cluster_id, member_order, cluster_slot, cluster_size):
    n = lax.axis_size("dev")
    nz, nq = split_lines(n)
    rows, depth = embeddings.shape
    clusters = cluster_slot.shape[0]
    per_owner = clusters // n
    width = min(CHUNK, depth // nz)
    chunks = depth // nz // width
    group = nz * per_owner
    slots = source_slots(n, nq, rows, group)
    pair = 2 if chunks % 2 == 0 else 1
    half = CAP // 2
    vmem = pl.BlockSpec(memory_space=pltpu.VMEM)
    dma = pltpu.SemaphoreType.DMA
    packed = pl.pallas_call(
        functools.partial(kernel, n, nz, nq),
        out_shape=pltpu.VMEM((8, rows), F32),
        in_specs=[pl.BlockSpec(memory_space=pl.ANY)] * 5,
        out_specs=vmem,
        scratch_shapes=[
            pltpu.VMEM((rows, depth), F32),
            pltpu.VMEM((1, rows), I32),
            pltpu.VMEM((1, rows), I32),
            pltpu.VMEM((1, clusters), I32),
            pltpu.VMEM((1, clusters), I32),
            pltpu.VMEM((nz, chunks, rows, width), BF16),
            pltpu.VMEM((chunks, nz, rows, width), BF16),
            pltpu.VMEM((nz, 8, rows), F32),
            pltpu.VMEM((nz, nq * slots, rows), BF16),
            pltpu.VMEM((chunks, nq - 1, nz * slots, width), BF16),
            pltpu.VMEM((chunks, nq, nz * slots, width), BF16),
            pltpu.VMEM((n, slots, width), BF16),
            pltpu.VMEM((nq, 8, nz * slots), F32),
            pltpu.VMEM((nq, 8, nz * slots), F32),
            pltpu.VMEM((group, half, CAP), F32),
            pltpu.VMEM((group, half, CAP), I16),
            pltpu.VMEM((nz, group // 2, half, CAP), I16),
            pltpu.VMEM((2 * nq, group // 2, CAP), F32),
            pltpu.VMEM((group // 2, 2 * CAP, pair * width), BF16),
            pltpu.VMEM((group, CAP, n * slots), BF16),
            dma((LOADS,)), dma((4,)), dma((chunks - STRAIGHT,)), dma((chunks - STRAIGHT,)), dma((7,)), dma((5,)),
        ],
        compiler_params=pltpu.CompilerParams(
            collective_id=0, has_side_effects=True, vmem_limit_bytes=62 * 1024 * 1024),
    )(embeddings, cluster_id.reshape(1, rows), member_order.reshape(1, rows),
      cluster_slot.reshape(1, clusters), cluster_size.reshape(1, clusters))
    best, keep, mean = pl.pallas_call(
        finish,
        out_shape=(jax.ShapeDtypeStruct((1, rows), F32), jax.ShapeDtypeStruct((1, rows), I32),
                   jax.ShapeDtypeStruct((1, per_owner), F32)),
        in_specs=[vmem],
        out_specs=(vmem,) * 3,
    )(pltpu.with_memory_space_constraint(packed, pltpu.VMEM))
    return best.reshape(rows), keep.reshape(rows), mean.reshape(per_owner)


def solution(mesh):
    placed = (P(("rep", "dev"), None), P(("rep", "dev")), P(("rep", "dev")), P("rep"), P("rep"))
    return jax.shard_map(
        body,
        mesh=mesh,
        in_specs=placed,
        out_specs=(P(("rep", "dev")), P(("rep", "dev")), P(("rep", "dev"))),
        check_vma=False,
    )
```
